32 devices in a mesh: rows: 4 (over z), tp: 4 (over y, x), unit: 2 (over core).
Axes of the slice: x: 2, y: 2, z: 4, core: 2. Of those that a mesh axis runs over, the one named last changes fastest.
Arguments:
- w_query: bfloat16 [5120, 4096], P(('unit', 'rows'), 'tp'), parts along dimension 0, may hold values from -0.125 to 0.125
- low_query: bfloat16 [5120, 64], P(('unit', 'rows')), parts along dimension 0, may hold values from -0.125 to 0.125
- high_query: bfloat16 [128, 4096], P('unit', 'tp'), parts along dimension 0, may hold values from -0.75 to 0.75
- w_key: bfloat16 [5120, 1024], P(('unit', 'rows'), 'tp'), parts along dimension 0, may hold values from -0.125 to 0.125
- low_key: bfloat16 [5120, 64], P(('unit', 'rows')), parts along dimension 0, may hold values from -0.125 to 0.125
- high_key: bfloat16 [128, 1024], P('unit', 'tp'), parts along dimension 0, may hold values from -0.75 to 0.75
- w_value: bfloat16 [5120, 1024], P(('unit', 'rows'), 'tp'), parts along dimension 0, may hold values from -0.125 to 0.125
- low_value: bfloat16 [5120, 64], P(('unit', 'rows')), parts along dimension 0, may hold values from -0.125 to 0.125
- high_value: bfloat16 [128, 1024], P('unit', 'tp'), parts along dimension 0, may hold values from -0.75 to 0.75
- w_mixed: bfloat16 [8192, 2560], P(('unit', 'tp'), 'rows'), parts along dimension 0, may hold values from -0.09375 to 0.09375
- low_mixed: bfloat16 [8192, 64], P(('unit', 'tp')), parts along dimension 0, may hold values from -0.09375 to 0.09375
- high_mixed: bfloat16 [128, 2560], P('unit', 'rows'), parts along dimension 0, may hold values from -0.75 to 0.75
- norm_train: float32 [5120], P(('unit', 'rows', 'tp')), parts along dimension 0, may hold values from 0.25 to 1.75
- norm_step: float32 [5120], P(('unit', 'rows', 'tp')), parts along dimension 0, may hold values from -0.3 to 0.3
Outputs:
- final_query: bfloat16 [5120, 4096], P('unit', 'tp'), parts along dimension 0
- final_key: bfloat16 [5120, 1024], P('unit', 'tp'), parts along dimension 0
- final_value: bfloat16 [5120, 1024], P('unit', 'tp'), parts along dimension 0
- final_mixed: bfloat16 [8192, 2560], P(('unit', 'tp')), parts along dimension 0
- serve_norm: bfloat16 [5120], P('unit'), parts along dimension 0
The draws below stay inside these ranges and needn't reach their ends.
There are 2 independent parts, one for each index of `unit`. The reference program is written for one: setup_inputs(seed, part) draws one part's arguments, and reference() takes and returns one part's arrays. A program takes and returns all parts, laid end to end along the dimension named above; each array names one. Nothing has to cross between parts.
All inputs are finite; a program needn't handle non-finite values.
Results may differ from the reference program's by a relative error of at most 0.001.
Values may be sent and summed in bfloat16 or wider, within the bound.
A program may use at most 128 MiB of HBM per device.

```python
import jax
import jax.numpy as jnp

D_MODEL = 2560
Q_DIM = 4096
KV_DIM = 1024
RANK = 64


def block_levels(own_key, dims, pieces, smallest, largest):
    gain, own = 1.0, jax.random.fold_in(own_key, 6)
    for position, parts in pieces:
        steps = jnp.exp(jax.random.uniform(jax.random.fold_in(own, position), (parts,), jnp.float32, smallest / len(pieces), largest / len(pieces)))
        gain = gain * jnp.repeat(steps, dims[position] // parts).reshape([-1 if axis == position else 1 for axis in range(len(dims))])
    return gain


def gaussian(stream_key, shape, deviation, limit, pieces=(), dtype=jnp.bfloat16):
    drawn = jax.random.normal(stream_key, shape, jnp.float32) * deviation
    if len(pieces) > 0:
        drawn = block_levels(stream_key, shape, pieces, -0.22, 0.18) * drawn
    return jnp.clip(drawn, min=-limit, max=limit).astype(dtype)


def setup_inputs(seed: int = 0, part: int = 0) -> dict:
    key_of = jax.random.split(jax.random.key(seed), 15)
    own_keys = jax.random.split(jax.random.fold_in(key_of[14], part), 15)
    return {
        "w_query": gaussian(own_keys[0], (D_MODEL, Q_DIM), D_MODEL ** -0.5, 0.125, ((0, 4), (1, 4))),
        "low_query": gaussian(own_keys[1], (D_MODEL, RANK), D_MODEL ** -0.5, 0.125, ((0, 4),)),
        "high_query": gaussian(own_keys[2], (RANK, Q_DIM), RANK ** -0.5, 0.75, ((1, 4),)),
        "w_key": gaussian(own_keys[3], (D_MODEL, KV_DIM), D_MODEL ** -0.5, 0.125, ((0, 4), (1, 4))),
        "low_key": gaussian(own_keys[4], (D_MODEL, RANK), D_MODEL ** -0.5, 0.125, ((0, 4),)),
        "high_key": gaussian(own_keys[5], (RANK, KV_DIM), RANK ** -0.5, 0.75, ((1, 4),)),
        "w_value": gaussian(own_keys[6], (D_MODEL, KV_DIM), D_MODEL ** -0.5, 0.125, ((0, 4), (1, 4))),
        "low_value": gaussian(own_keys[7], (D_MODEL, RANK), D_MODEL ** -0.5, 0.125, ((0, 4),)),
        "high_value": gaussian(own_keys[8], (RANK, KV_DIM), RANK ** -0.5, 0.75, ((1, 4),)),
        "w_mixed": gaussian(own_keys[9], (Q_DIM, D_MODEL), Q_DIM ** -0.5, 0.09375, ((0, 4), (1, 4))),
        "low_mixed": gaussian(own_keys[10], (Q_DIM, RANK), Q_DIM ** -0.5, 0.09375, ((0, 4),)),
        "high_mixed": gaussian(own_keys[11], (RANK, D_MODEL), RANK ** -0.5, 0.75, ((1, 4),)),
        "norm_train": jnp.clip(1.0 + 0.15 * jax.random.normal(own_keys[12], (D_MODEL,), jnp.float32), 0.25, 1.75),
        "norm_step": jnp.clip(jax.random.uniform(own_keys[13], (D_MODEL,), jnp.float32, -0.3, 0.3) * block_levels(own_keys[13], (D_MODEL,), ((0, 16),), -0.4, 0.0), -0.3, 0.3),
    }


mix_rate = 0.5


def reference(w_query, low_query, high_query, w_key, low_key, high_key, w_value, low_value, high_value, w_mixed, low_mixed, high_mixed, norm_train, norm_step):
    result_query = w_query.astype(jnp.float32) + mix_rate * jnp.dot(low_query, high_query, preferred_element_type=jnp.float32)
    result_key = w_key.astype(jnp.float32) + mix_rate * jnp.dot(low_key, high_key, preferred_element_type=jnp.float32)
    result_value = w_value.astype(jnp.float32) + mix_rate * jnp.dot(low_value, high_value, preferred_element_type=jnp.float32)
    result_mixed = w_mixed.astype(jnp.float32) + mix_rate * jnp.dot(low_mixed, high_mixed, preferred_element_type=jnp.float32)
    final_query = result_query.astype(jnp.bfloat16)
    final_key = result_key.astype(jnp.bfloat16)
    final_value = result_value.astype(jnp.bfloat16)
    final_mixed = result_mixed.astype(jnp.bfloat16)
    serve_norm = (norm_train + norm_step).astype(jnp.bfloat16)
    return final_query, final_key, final_value, final_mixed, serve_norm
```

```python
import functools

import jax
import jax.numpy as jnp
from jax import lax
from jax.experimental import pallas as pl
from jax.experimental.pallas import tpu as pltpu
from jax.sharding import PartitionSpec as P

MESH = pl.DeviceIdType.MESH
mix_rate = 0.5
order = (1, 0, 3, 2)
late_kind = order[-1]


def pieces_of(rows, firsts):
    sizes = [size for size in firsts if sum(firsts) < rows]
    left = rows - sum(sizes)
    return [*sizes, left] if left % 16 == 0 or not sizes else [rows]


def rounds_of(tps, t):
    if tps & (tps - 1):
        return [[(lax.rem(t + step, tps), t, lax.rem(t + tps - step, tps), 1) for step in range(1, tps)]]
    rounds, size = [], 1
    while size < tps:
        side = lax.rem(t // size, 2)
        base = (t // size) * size
        across = size - 2 * size * side
        rounds.append([(t + across, base, base + across, size)])
        size *= 2
    return rounds


def block_of(size, options):
    for option in options:
        if size % option == 0:
            return option
    return size


def kernel(n, tps, units, stacked, pieces, *refs):
    kinds = len(pieces)
    w, low, high = refs[:kinds], refs[kinds : 2 * kinds], refs[2 * kinds : 3 * kinds]
    norm_train, norm_step = refs[3 * kinds : 3 * kinds + 2]
    refs = refs[3 * kinds + 2 :]
    out, norm_out = refs[:kinds], refs[kinds]
    refs = refs[kinds + 1 :]
    w_own, low_own, high_own = refs[:kinds], refs[kinds : 2 * kinds], refs[2 * kinds : 3 * kinds]
    low_rows = refs[3 * kinds : 4 * kinds]
    refs = refs[4 * kinds :]
    norm_own, norm_all, norm_sem, load_sem, side_sem, send_sem, recv_sem, pass_send, pass_recv, norm_send, norm_recv, cross_send, cross_recv = refs

    z, t = lax.axis_index("rows"), lax.axis_index("tp")
    late = lax.axis_index("unit") == units - 1
    rounds = rounds_of(tps, t)
    chunks = [(k, p) for k in order for p in range(len(pieces[k]))]
    has_up, has_down = z < n - 1, z > 0
    held_up, held_down = late & (z == n - 2), late & (z == 1)
    missing_up, missing_down = late & (z == n - 1), late & (z == 0)

    def sends(k, direction):
        has, held = ((has_up, held_up), (has_down, held_down))[direction]
        return has & ~held if k == late_kind else has

    def comes(k, d, direction):
        has, missing = ((z - d >= 0, missing_up), (z + d < n, missing_down))[direction]
        return has & ~missing if k == late_kind else has

    def rows_of(k, p):
        return sum(pieces[k][:p]), pieces[k][p]

    def load(i):
        k, p = chunks[i]
        start, size = rows_of(k, p)
        return pltpu.make_async_copy(
            w[k].at[pl.ds(start, size)], w_own[k].at[pl.ds(start, size)], load_sem.at[i]
        )

    def side(k):
        return (
            pltpu.make_async_copy(low[k], low_own[k], side_sem.at[0, k]),
            pltpu.make_async_copy(high[k], high_own[k], side_sem.at[1, k]),
        )

    def load_kind(kind):
        for copy in side(kind):
            copy.start()
        for i, (k, p) in enumerate(chunks):
            if k == kind:
                load(i).start()

    load_kind(order[0])

    barrier = pltpu.get_barrier_semaphore()

    @pl.when(has_up)
    def _():
        pl.semaphore_signal(barrier, inc=1, device_id={"rows": z + 1}, device_id_type=MESH)

    @pl.when(has_down)
    def _():
        pl.semaphore_signal(barrier, inc=1, device_id={"rows": z - 1}, device_id_type=MESH)

    for partner in [exchange[0] for exchanges in rounds for exchange in exchanges]:
        pl.semaphore_signal(barrier, inc=1, device_id={"tp": partner}, device_id_type=MESH)

    for kind in order[1:]:
        load_kind(kind)

    norm_loads = [
        pltpu.make_async_copy(source, norm_own.at[j], norm_sem.at[j])
        for j, source in enumerate((norm_train, norm_step))
    ]
    for copy in norm_loads:
        copy.start()

    def region(k, p, origin):
        start, size = (0, w[k].shape[0]) if p is None else rows_of(k, p)
        columns = w[k].shape[1]
        if stacked[k]:
            return out[k].at[origin, pl.ds(start, size)]
        if out[k].shape[1] == columns:
            rows = w[k].shape[0]
            return out[k].at[pl.ds(pl.multiple_of(origin * rows + start, 16), size)]
        return out[k].at[pl.ds(start, size), pl.ds(pl.multiple_of(origin * columns, 128), columns)]

    def hop(place, send, recv, direction):
        return pltpu.make_async_remote_copy(
            src_ref=place,
            dst_ref=place,
            send_sem=send,
            recv_sem=recv,
            device_id={"rows": z + 1 - 2 * direction},
            device_id_type=MESH,
        )

    def chunk_hop(i, origin, direction):
        k, p = chunks[i]
        return hop(region(k, p, origin), send_sem.at[direction, i], recv_sem.at[direction, i], direction)

    def whole_hop(k, origin, direction):
        return hop(
            region(k, None, origin),
            pass_send.at[direction, origin, k],
            pass_recv.at[direction, origin, k],
            direction,
        )

    def norm_hop(origin, direction):
        return pltpu.make_async_remote_copy(
            src_ref=norm_all.at[origin, t],
            dst_ref=norm_all.at[origin, t],
            send_sem=norm_send.at[direction, origin],
            recv_sem=norm_recv.at[direction, origin],
            device_id={"rows": z + 1 - 2 * direction},
            device_id_type=MESH,
        )

    def cross(r, j, coming=False):
        partner, base, theirs, size = rounds[r][j]
        place = norm_all.at[:, pl.ds(theirs if coming else base, size)]
        return pltpu.make_async_remote_copy(
            src_ref=place,
            dst_ref=place,
            send_sem=cross_send.at[r, j],
            recv_sem=cross_recv.at[r, j],
            device_id={"tp": partner},
            device_id_type=MESH,
        )

    def cross_start(r):
        for j in range(len(rounds[r])):
            cross(r, j).start()

    def cross_wait(r):
        for j in range(len(rounds[r])):
            cross(r, j, coming=True).wait_recv()

    def send_both(make, k=None):
        for direction in range(2):

            @pl.when(sends(k, direction))
            def _():
                make(direction).start()

    def merge(i):
        k, p = chunks[i]
        start, size = rows_of(k, p)
        columns = w[k].shape[1]
        high_block = block_of(size, (160, 128, 64, 32, 16))
        wide_block = block_of(columns, (256, 128))
        wides = columns // wide_block
        place = region(k, p, z)

        def body(b, _):
            if size == high_block:
                r, c = 0, b
            else:
                r, c = b // wides, b % wides
            r = r * high_block
            c = 0 if wides == 1 else pl.multiple_of(c * wide_block, wide_block)
            mine = pl.ds(start + r, high_block)
            wide = pl.ds(c, wide_block)
            result = w_own[k][mine, wide].astype(jnp.float32) + mix_rate * jnp.dot(
                low_rows[k][mine, :], high_own[k][:, wide], preferred_element_type=jnp.float32
            )
            place[pl.ds(r, high_block), wide] = result.astype(jnp.bfloat16)
            return 0

        lax.fori_loop(0, (size // high_block) * wides, body, 0)

    for i, (k, p) in enumerate(chunks):
        if p == 0:
            for copy in side(k):
                copy.wait()
            low_rows[k][...] = low_own[k][...].astype(jnp.float32).T.astype(jnp.bfloat16)
        load(i).wait()
        merge(i)
        if i == 1:
            partners = has_up.astype(jnp.int32) + has_down.astype(jnp.int32) + sum(map(len, rounds))
            pl.semaphore_wait(barrier, partners)
        if i > 0:
            send_both(functools.partial(chunk_hop, i - 1, z), chunks[i - 1][0])
        if i == min(3, len(chunks) - 2):
            for copy in norm_loads:
                copy.wait()
            norm_all[z, t] = (norm_own[0] + norm_own[1]).astype(jnp.bfloat16).astype(jnp.float32)
        if i == min(4, len(chunks) - 1):
            send_both(functools.partial(norm_hop, z))
    send_both(functools.partial(chunk_hop, len(chunks) - 1, z), chunks[-1][0])

    def arrival(arrived, onward, d, k=None):
        for direction, origin in ((0, z - d), (1, z + d)):

            @pl.when(comes(k, d, direction))
            def _():
                for make in arrived:
                    make(origin, direction).wait_recv()

                @pl.when(sends(k, direction))
                def _():
                    onward(origin, direction).start()

    def distance(d, _, near=False):
        arrival([norm_hop], norm_hop, d)

        @pl.when(d == n - 1)
        def _():
            cross_start(0)

        for j, k in enumerate(order):
            onward = functools.partial(whole_hop, k)
            arrived = [onward]
            if near:
                arrived = [functools.partial(chunk_hop, i) for i, c in enumerate(chunks) if c[0] == k]
            if k == order[-1]:

                @pl.when(d == n - 1)
                def _():
                    all_norms()

            arrival(arrived, onward, d, k)
        return 0

    def all_norms():
        for r in range(len(rounds)):
            if r > 0:
                cross_start(r)
            cross_wait(r)
        line = jnp.concatenate([norm_all[a, b] for a in range(n) for b in range(tps)], axis=1)
        width = norm_out.shape[1]
        norm_out[...] = jnp.concatenate(
            [line[:, a * width : (a + 1) * width] for a in range(norm_out.shape[0])], axis=0
        ).astype(jnp.bfloat16)

    distance(jnp.int32(1), 0, near=True)
    lax.fori_loop(2, n, distance, 0)

    for direction in range(2):
        for i in range(len(chunks)):

            @pl.when(sends(chunks[i][0], direction))
            def _():
                chunk_hop(i, z, direction).wait_send()

        @pl.when(sends(None, direction))
        def _():
            norm_hop(z, direction).wait_send()

    def drain(origin, _):
        for direction, passed in ((0, origin < z), (1, origin > z)):
            for k in range(kinds):

                @pl.when(sends(k, direction) & passed)
                def _():
                    whole_hop(k, origin, direction).wait_send()

            @pl.when(sends(None, direction) & passed)
            def _():
                norm_hop(origin, direction).wait_send()

        return 0

    lax.fori_loop(0, n, drain, 0)
    for r in range(len(rounds)):
        for j in range(len(rounds[r])):
            cross(r, j).wait_send()


def ends(n, units):
    z, late = lax.axis_index("rows"), lax.axis_index("unit") == units - 1
    return late & (z == 0), late & (z == n - 1)


def put(n, units, parts, *refs):
    kinds = len(parts)
    src, dst, sem = refs[:kinds], refs[kinds : 2 * kinds], refs[-1]
    bottom, top = ends(n, units)
    copies, kept = [], []
    for k in range(kinds):
        size = src[k].shape[0] // parts[k]
        for p in range(parts[k]):
            rows = pl.ds(p * size, size)
            copy = pltpu.make_async_copy(src[k].at[rows], dst[k].at[rows], sem.at[len(copies) + len(kept)])
            (kept if k == late_kind else copies).append(copy)
    share = src[late_kind].shape[0] // n

    def own(origin):
        rows = pl.ds(origin * share, share)
        return pltpu.make_async_copy(src[late_kind].at[rows], dst[late_kind].at[rows], sem.at[sum(parts)])

    for copy in copies:
        copy.start()

    @pl.when(~bottom & ~top)
    def _():
        for copy in kept:
            copy.start()
        for copy in kept:
            copy.wait()

    for flag, origin in ((bottom, 0), (top, n - 1)):

        @pl.when(flag)
        def _():
            own(origin).start()
            own(origin).wait()

    for copy in copies:
        copy.wait()


def place(n, units, arrays):
    parts = [2 if x.shape[0] % 128 == 0 else 1 for x in arrays]
    vmem, hbm = pl.BlockSpec(memory_space=pltpu.VMEM), pl.BlockSpec(memory_space=pltpu.HBM)
    return pl.pallas_call(
        functools.partial(put, n, units, parts),
        out_shape=[pltpu.HBM(x.shape, x.dtype) for x in arrays] + [pltpu.VMEM((8, 128), jnp.float32)],
        in_specs=[vmem] * len(arrays),
        out_specs=[hbm] * len(arrays) + [vmem],
        scratch_shapes=[pltpu.SemaphoreType.DMA((sum(parts) + 1,))],
        compiler_params=pltpu.CompilerParams(vmem_limit_bytes=24 * 1024 * 1024),
        name="place",
    )(*arrays)


def last_hop(n, units, have, after, got, send_sem, recv_sem):
    z, late = lax.axis_index("rows"), lax.axis_index("unit") == units - 1
    bottom, top = ends(n, units)
    size = got.shape[0]
    share = have.shape[0] - size

    def hop(direction):
        return pltpu.make_async_remote_copy(
            src_ref=have.at[pl.ds(share * direction, size)],
            dst_ref=got,
            send_sem=send_sem.at[direction],
            recv_sem=recv_sem.at[direction],
            device_id={"rows": z + 1 - 2 * direction},
            device_id_type=MESH,
        )

    barrier = pltpu.get_barrier_semaphore()
    above, below = late & (z == n - 2), late & (z == 1)

    @pl.when(bottom)
    def _():
        pl.semaphore_signal(barrier, inc=1, device_id={"rows": z + 1}, device_id_type=MESH)

    @pl.when(top)
    def _():
        pl.semaphore_signal(barrier, inc=1, device_id={"rows": z - 1}, device_id_type=MESH)

    @pl.when(above | below)
    def _():
        pl.semaphore_wait(barrier, above.astype(jnp.int32) + below.astype(jnp.int32))

    for direction, flag in ((0, above), (1, below)):

        @pl.when(flag)
        def _():
            hop(direction).start()

    for direction, flag in ((0, top), (1, bottom)):

        @pl.when(flag)
        def _():
            hop(direction).wait_recv()

    for direction, flag in ((0, above), (1, below)):

        @pl.when(flag)
        def _():
            hop(direction).wait_send()


def finish(n, units, have, after):
    share = have.shape[0] // n
    vmem, dma = pl.BlockSpec(memory_space=pltpu.VMEM), pltpu.SemaphoreType.DMA
    return pl.pallas_call(
        functools.partial(last_hop, n, units),
        out_shape=pltpu.VMEM((have.shape[0] - share, have.shape[1]), have.dtype),
        in_specs=[vmem, vmem],
        out_specs=vmem,
        scratch_shapes=[dma((2,)), dma((2,))],
        compiler_params=pltpu.CompilerParams(
            collective_id=1, has_side_effects=True, vmem_limit_bytes=4 * 1024 * 1024
        ),
        name="last_hop",
    )(have, after)


def add_rows(n, units, got, old, out, sem):
    size = got.shape[0]
    share = out.shape[0] - size
    for flag, start in zip(ends(n, units), (share, 0)):

        @pl.when(flag)
        def _():
            copy = pltpu.make_async_copy(got, out.at[pl.ds(start, size)], sem)
            copy.start()
            copy.wait()


def complete(n, units, got, old):
    vmem, hbm = pl.BlockSpec(memory_space=pltpu.VMEM), pl.BlockSpec(memory_space=pltpu.HBM)
    return pl.pallas_call(
        functools.partial(add_rows, n, units),
        out_shape=pltpu.HBM(old.shape, old.dtype),
        in_specs=[vmem, hbm],
        out_specs=hbm,
        scratch_shapes=[pltpu.SemaphoreType.DMA],
        input_output_aliases={1: 0},
        compiler_params=pltpu.CompilerParams(vmem_limit_bytes=4 * 1024 * 1024),
        name="complete",
    )(got, old)


def shards(n, tps, units, *args):
    w, low, high = args[0:12:3], [x.T for x in args[1:12:3]], args[2:12:3]
    norm_train, norm_step = args[12].reshape(1, -1), args[13].reshape(1, -1)
    kinds = len(w)
    by_column = [False] * (kinds - 1) + [True]
    stacked = [by_column[k] and w[k].shape[1] % 128 != 0 for k in range(kinds)]
    firsts = {order[0]: (64, 128), order[1]: (160,)}
    pieces = [pieces_of(w[k].shape[0], firsts.get(k, ())) for k in range(kinds)]
    count = sum(map(len, pieces))
    shapes = []
    for k in range(kinds):
        rows, columns = w[k].shape
        if stacked[k]:
            shapes.append((n, rows, columns))
        elif by_column[k]:
            shapes.append((rows, n * columns))
        else:
            shapes.append((n * rows, columns))
    share = norm_train.shape[1]
    total = n * tps * share
    width = 128 if total % 128 == 0 else total
    vmem, hbm = pl.BlockSpec(memory_space=pltpu.VMEM), pl.BlockSpec(memory_space=pltpu.HBM)
    dma = pltpu.SemaphoreType.DMA
    operands = (*w, *low, *high, norm_train, norm_step)
    results = pl.pallas_call(
        functools.partial(kernel, n, tps, units, stacked, pieces),
        out_shape=[pltpu.VMEM(s, jnp.bfloat16) for s in shapes]
        + [pltpu.VMEM((total // width, width), jnp.bfloat16)],
        in_specs=[hbm] * (3 * kinds + 2),
        out_specs=[vmem] * (kinds + 1),
        scratch_shapes=[pltpu.VMEM(x.shape, x.dtype) for x in (*w, *low, *high)]
        + [pltpu.VMEM(x.shape[::-1], x.dtype) for x in low]
        + [
            pltpu.VMEM((2, 1, share), jnp.float32),
            pltpu.VMEM((n, tps, 1, share), jnp.float32),
            dma((2,)),
            dma((count,)),
            dma((2, kinds)),
            dma((2, count)),
            dma((2, count)),
            dma((2, n, kinds)),
            dma((2, n, kinds)),
            dma((2, n)),
            dma((2, n)),
            dma((tps, tps)),
            dma((tps, tps)),
        ],
        compiler_params=pltpu.CompilerParams(
            collective_id=0, has_side_effects=True, vmem_limit_bytes=24 * 1024 * 1024
        ),
        name="merge_and_gather",
    )(*[pltpu.with_memory_space_constraint(x, pltpu.HBM) for x in operands])
    have = results[late_kind]
    *results, after = place(n, units, results)
    if n > 1:
        results[late_kind] = complete(n, units, finish(n, units, have, after), results[late_kind])
    finals = []
    for k in range(kinds):
        full = results[k]
        if stacked[k]:
            full = full.transpose(1, 0, 2).reshape(full.shape[1], -1)
        finals.append(full)
    return (*finals, results[kinds].reshape(-1))


def solution(mesh):
    return jax.shard_map(
        functools.partial(shards, mesh.shape["rows"], mesh.shape["tp"], mesh.shape["unit"]),
        mesh=mesh,
        in_specs=(
            P(("unit", "rows"), "tp"),
            P(("unit", "rows"), None),
            P("unit", "tp"),
            P(("unit", "rows"), "tp"),
            P(("unit", "rows"), None),
            P("unit", "tp"),
            P(("unit", "rows"), "tp"),
            P(("unit", "rows"), None),
            P("unit", "tp"),
            P(("unit", "tp"), "rows"),
            P(("unit", "tp"), None),
            P("unit", "rows"),
            P(("unit", "rows", "tp")),
            P(("unit", "rows", "tp")),
        ),
        out_specs=(
            P("unit", "tp"),
            P("unit", "tp"),
            P("unit", "tp"),
            P(("unit", "tp"), None),
            P("unit"),
        ),
        check_vma=False,
    )
```

```python
import functools

import jax
import jax.numpy as jnp
from jax import lax
from jax.experimental import pallas as pl
from jax.experimental.pallas import tpu as pltpu
from jax.sharding import PartitionSpec as P

MESH = pl.DeviceIdType.MESH
mix_rate = 0.5
order = (1, 0, 3, 2)
late_kind = order[-1]


def pieces_of(rows, firsts):
    sizes = [size for size in firsts if sum(firsts) < rows]
    left = rows - sum(sizes)
    return [*sizes, left] if left % 16 == 0 or not sizes else [rows]


def rounds_of(tps, t):
    if tps & (tps - 1):
        return [[(lax.rem(t + step, tps), t, lax.rem(t + tps - step, tps), 1) for step in range(1, tps)]]
    rounds, size = [], 1
    while size < tps:
        side = lax.rem(t // size, 2)
        base = (t // size) * size
        across = size - 2 * size * side
        rounds.append([(t + across, base, base + across, size)])
        size *= 2
    return rounds


def block_of(size, options):
    for option in options:
        if size % option == 0:
            return option
    return size


def kernel(n, tps, units, stacked, pieces, *refs):
    kinds = len(pieces)
    w, low, high = refs[:kinds], refs[kinds : 2 * kinds], refs[2 * kinds : 3 * kinds]
    norm_train, norm_step = refs[3 * kinds : 3 * kinds + 2]
    refs = refs[3 * kinds + 2 :]
    out, norm_out = refs[:kinds], refs[kinds]
    refs = refs[kinds + 1 :]
    w_own, low_own, high_own = refs[:kinds], refs[kinds : 2 * kinds], refs[2 * kinds : 3 * kinds]
    low_rows = refs[3 * kinds : 4 * kinds]
    refs = refs[4 * kinds :]
    norm_own, norm_all, norm_sem, load_sem, side_sem, send_sem, recv_sem, pass_send, pass_recv, norm_send, norm_recv, cross_send, cross_recv = refs

    z, t = lax.axis_index("rows"), lax.axis_index("tp")
    late = lax.axis_index("unit") == units - 1
    rounds = rounds_of(tps, t)
    chunks = [(k, p) for k in order for p in range(len(pieces[k]))]
    has_up, has_down = z < n - 1, z > 0
    held_up, held_down = late & (z == n - 2), late & (z == 1)
    missing_up, missing_down = late & (z == n - 1), late & (z == 0)

    def sends(k, direction):
        has, held = ((has_up, held_up), (has_down, held_down))[direction]
        return has & ~held if k == late_kind else has

    def comes(k, d, direction):
        has, missing = ((z - d >= 0, missing_up), (z + d < n, missing_down))[direction]
        return has & ~missing if k == late_kind else has

    def rows_of(k, p):
        return sum(pieces[k][:p]), pieces[k][p]

    def load(i):
        k, p = chunks[i]
        start, size = rows_of(k, p)
        return pltpu.make_async_copy(
            w[k].at[pl.ds(start, size)], w_own[k].at[pl.ds(start, size)], load_sem.at[i]
        )

    def side(k):
        return (
            pltpu.make_async_copy(low[k], low_own[k], side_sem.at[0, k]),
            pltpu.make_async_copy(high[k], high_own[k], side_sem.at[1, k]),
        )

    def load_kind(kind):
        for copy in side(kind):
            copy.start()
        for i, (k, p) in enumerate(chunks):
            if k == kind:
                load(i).start()

    barrier = pltpu.get_barrier_semaphore()

    @pl.when(has_up)
    def _():
        pl.semaphore_signal(barrier, inc=1, device_id={"rows": z + 1}, device_id_type=MESH)

    @pl.when(has_down)
    def _():
        pl.semaphore_signal(barrier, inc=1, device_id={"rows": z - 1}, device_id_type=MESH)

    for partner in [exchange[0] for exchanges in rounds for exchange in exchanges]:
        pl.semaphore_signal(barrier, inc=1, device_id={"tp": partner}, device_id_type=MESH)

    for kind in order:
        load_kind(kind)

    norm_loads = [
        pltpu.make_async_copy(source, norm_own.at[j], norm_sem.at[j])
        for j, source in enumerate((norm_train, norm_step))
    ]
    for copy in norm_loads:
        copy.start()

    def region(k, p, origin):
        start, size = (0, w[k].shape[0]) if p is None else rows_of(k, p)
        columns = w[k].shape[1]
        if stacked[k]:
            return out[k].at[origin, pl.ds(start, size)]
        if out[k].shape[1] == columns:
            rows = w[k].shape[0]
            return out[k].at[pl.ds(pl.multiple_of(origin * rows + start, 16), size)]
        return out[k].at[pl.ds(start, size), pl.ds(pl.multiple_of(origin * columns, 128), columns)]

    def hop(place, send, recv, direction):
        return pltpu.make_async_remote_copy(
            src_ref=place,
            dst_ref=place,
            send_sem=send,
            recv_sem=recv,
            device_id={"rows": z + 1 - 2 * direction},
            device_id_type=MESH,
        )

    def chunk_hop(i, origin, direction):
        k, p = chunks[i]
        return hop(region(k, p, origin), send_sem.at[direction, i], recv_sem.at[direction, i], direction)

    def whole_hop(k, origin, direction):
        return hop(
            region(k, None, origin),
            pass_send.at[origin, k],
            pass_recv.at[origin, k],
            direction,
        )

    def norm_hop(origin, direction, own=0):
        return pltpu.make_async_remote_copy(
            src_ref=norm_all.at[origin, t],
            dst_ref=norm_all.at[origin, t],
            send_sem=norm_send.at[own * direction, origin],
            recv_sem=norm_recv.at[origin],
            device_id={"rows": z + 1 - 2 * direction},
            device_id_type=MESH,
        )

    def cross(r, j, coming=False):
        partner, base, theirs, size = rounds[r][j]
        place = norm_all.at[:, pl.ds(theirs if coming else base, size)]
        return pltpu.make_async_remote_copy(
            src_ref=place,
            dst_ref=place,
            send_sem=cross_send.at[r, j],
            recv_sem=cross_recv.at[r, j],
            device_id={"tp": partner},
            device_id_type=MESH,
        )

    def cross_start(r):
        for j in range(len(rounds[r])):
            cross(r, j).start()

    def cross_wait(r):
        for j in range(len(rounds[r])):
            cross(r, j, coming=True).wait_recv()

    def send_both(make, k=None):
        for direction in range(2):

            @pl.when(sends(k, direction))
            def _():
                make(direction).start()

    def merge(i):
        k, p = chunks[i]
        start, size = rows_of(k, p)
        columns = w[k].shape[1]
        high_block = block_of(size, (160, 128, 64, 32, 16))
        wide_block = block_of(columns, (256, 128))
        wides = columns // wide_block
        place = region(k, p, z)

        def body(b, _):
            if size == high_block:
                r, c = 0, b
            else:
                r, c = b // wides, b % wides
            r = r * high_block
            c = 0 if wides == 1 else pl.multiple_of(c * wide_block, wide_block)
            mine = pl.ds(start + r, high_block)
            wide = pl.ds(c, wide_block)
            result = w_own[k][mine, wide].astype(jnp.float32) + mix_rate * jnp.dot(
                low_rows[k][mine, :], high_own[k][:, wide], preferred_element_type=jnp.float32
            )
            place[pl.ds(r, high_block), wide] = result.astype(jnp.bfloat16)
            return 0

        lax.fori_loop(0, (size // high_block) * wides, body, 0)

    for i, (k, p) in enumerate(chunks):
        if p == 0:
            for copy in side(k):
                copy.wait()
        mine = pl.ds(*rows_of(k, p))
        low_rows[k][mine, :] = low_own[k][:, mine].astype(jnp.float32).T.astype(jnp.bfloat16)
        load(i).wait()
        merge(i)
        if i == 1:
            partners = has_up.astype(jnp.int32) + has_down.astype(jnp.int32) + sum(map(len, rounds))
            pl.semaphore_wait(barrier, partners)
        if i > 0:
            send_both(functools.partial(chunk_hop, i - 1, z), chunks[i - 1][0])
        if i == min(3, len(chunks) - 2):
            for copy in norm_loads:
                copy.wait()
            norm_all[z, t] = (norm_own[0] + norm_own[1]).astype(jnp.bfloat16).astype(jnp.float32)
        if i == min(4, len(chunks) - 1):
            send_both(functools.partial(norm_hop, z, own=1))
    send_both(functools.partial(chunk_hop, len(chunks) - 1, z), chunks[-1][0])

    def arrival(arrived, onward, d, k=None):
        for direction, origin in ((0, z - d), (1, z + d)):

            @pl.when(comes(k, d, direction))
            def _():
                for make in arrived:
                    make(origin, direction).wait_recv()

                @pl.when(sends(k, direction))
                def _():
                    onward(origin, direction).start()

    def distance(d, _, near=False):
        arrival([norm_hop], norm_hop, d)
        for j, k in enumerate(order):

            @pl.when(d == n - 1)
            def _():
                norm_round(j)

            onward = functools.partial(whole_hop, k)
            arrived = [onward]
            if near:
                arrived = [functools.partial(chunk_hop, i) for i, c in enumerate(chunks) if c[0] == k]
            arrival(arrived, onward, d, k)
        return 0

    def norm_round(j):
        last = len(rounds)
        if 0 < j <= last:
            cross_wait(j - 1)
        if j < last:
            cross_start(j)
        if j == min(last, kinds - 1):
            for r in range(j, last):
                cross_wait(r)
                if r + 1 < last:
                    cross_start(r + 1)
            write_norm()

    def write_norm():
        line = jnp.concatenate([norm_all[a, b] for a in range(n) for b in range(tps)], axis=1)
        width = norm_out.shape[1]
        norm_out[...] = jnp.concatenate(
            [line[:, a * width : (a + 1) * width] for a in range(norm_out.shape[0])], axis=0
        ).astype(jnp.bfloat16)

    distance(jnp.int32(1), 0, near=True)
    lax.fori_loop(2, n, distance, 0)

    for direction in range(2):
        for i in range(len(chunks)):

            @pl.when(sends(chunks[i][0], direction))
            def _():
                chunk_hop(i, z, direction).wait_send()

        @pl.when(sends(None, direction))
        def _():
            norm_hop(z, direction, own=1).wait_send()

    def drain(origin, _):
        for direction, passed in ((0, origin < z), (1, origin > z)):
            for k in range(kinds):

                @pl.when(sends(k, direction) & passed)
                def _():
                    whole_hop(k, origin, direction).wait_send()

            @pl.when(sends(None, direction) & passed)
            def _():
                norm_hop(origin, direction).wait_send()

        return 0

    lax.fori_loop(0, n, drain, 0)
    for r in range(len(rounds)):
        for j in range(len(rounds[r])):
            cross(r, j).wait_send()


def ends(n, units):
    z, late = lax.axis_index("rows"), lax.axis_index("unit") == units - 1
    return late & (z == 0), late & (z == n - 1)


def put(n, units, parts, *refs):
    kinds = len(parts)
    src, dst, sem = refs[:kinds], refs[kinds : 2 * kinds], refs[-1]
    bottom, top = ends(n, units)
    copies, kept = [], []
    for k in range(kinds):
        size = src[k].shape[0] // parts[k]
        for p in range(parts[k]):
            rows = pl.ds(p * size, size)
            copy = pltpu.make_async_copy(src[k].at[rows], dst[k].at[rows], sem.at[len(copies) + len(kept)])
            (kept if k == late_kind else copies).append(copy)
    share = src[late_kind].shape[0] // n

    def own(origin):
        rows = pl.ds(origin * share, share)
        return pltpu.make_async_copy(src[late_kind].at[rows], dst[late_kind].at[rows], sem.at[sum(parts)])

    for copy in copies:
        copy.start()

    @pl.when(~bottom & ~top)
    def _():
        for copy in kept:
            copy.start()
        for copy in kept:
            copy.wait()

    for flag, origin in ((bottom, 0), (top, n - 1)):

        @pl.when(flag)
        def _():
            own(origin).start()
            own(origin).wait()

    for copy in copies:
        copy.wait()


def place(n, units, arrays):
    parts = [2 if x.shape[0] % 128 == 0 else 1 for x in arrays]
    vmem, hbm = pl.BlockSpec(memory_space=pltpu.VMEM), pl.BlockSpec(memory_space=pltpu.HBM)
    return pl.pallas_call(
        functools.partial(put, n, units, parts),
        out_shape=[pltpu.HBM(x.shape, x.dtype) for x in arrays] + [pltpu.VMEM((8, 128), jnp.float32)],
        in_specs=[vmem] * len(arrays),
        out_specs=[hbm] * len(arrays) + [vmem],
        scratch_shapes=[pltpu.SemaphoreType.DMA((sum(parts) + 1,))],
        compiler_params=pltpu.CompilerParams(vmem_limit_bytes=24 * 1024 * 1024),
        name="place",
    )(*arrays)


def last_hop(n, units, have, after, got, send_sem, recv_sem):
    z, late = lax.axis_index("rows"), lax.axis_index("unit") == units - 1
    bottom, top = ends(n, units)
    size = got.shape[0]
    share = have.shape[0] - size

    def hop(direction):
        return pltpu.make_async_remote_copy(
            src_ref=have.at[pl.ds(share * direction, size)],
            dst_ref=got,
            send_sem=send_sem.at[direction],
            recv_sem=recv_sem.at[direction],
            device_id={"rows": z + 1 - 2 * direction},
            device_id_type=MESH,
        )

    barrier = pltpu.get_barrier_semaphore()
    above, below = late & (z == n - 2), late & (z == 1)

    @pl.when(bottom)
    def _():
        pl.semaphore_signal(barrier, inc=1, device_id={"rows": z + 1}, device_id_type=MESH)

    @pl.when(top)
    def _():
        pl.semaphore_signal(barrier, inc=1, device_id={"rows": z - 1}, device_id_type=MESH)

    @pl.when(above | below)
    def _():
        pl.semaphore_wait(barrier, above.astype(jnp.int32) + below.astype(jnp.int32))

    for direction, flag in ((0, above), (1, below)):

        @pl.when(flag)
        def _():
            hop(direction).start()

    for direction, flag in ((0, top), (1, bottom)):

        @pl.when(flag)
        def _():
            hop(direction).wait_recv()

    for direction, flag in ((0, above), (1, below)):

        @pl.when(flag)
        def _():
            hop(direction).wait_send()


def finish(n, units, have, after):
    share = have.shape[0] // n
    vmem, dma = pl.BlockSpec(memory_space=pltpu.VMEM), pltpu.SemaphoreType.DMA
    return pl.pallas_call(
        functools.partial(last_hop, n, units),
        out_shape=pltpu.VMEM((have.shape[0] - share, have.shape[1]), have.dtype),
        in_specs=[vmem, vmem],
        out_specs=vmem,
        scratch_shapes=[dma((2,)), dma((2,))],
        compiler_params=pltpu.CompilerParams(
            collective_id=1, has_side_effects=True, vmem_limit_bytes=4 * 1024 * 1024
        ),
        name="last_hop",
    )(have, after)


def add_rows(n, units, got, old, out, sem):
    size = got.shape[0]
    share = out.shape[0] - size
    for flag, start in zip(ends(n, units), (share, 0)):

        @pl.when(flag)
        def _():
            copy = pltpu.make_async_copy(got, out.at[pl.ds(start, size)], sem)
            copy.start()
            copy.wait()


def complete(n, units, got, old):
    vmem, hbm = pl.BlockSpec(memory_space=pltpu.VMEM), pl.BlockSpec(memory_space=pltpu.HBM)
    return pl.pallas_call(
        functools.partial(add_rows, n, units),
        out_shape=pltpu.HBM(old.shape, old.dtype),
        in_specs=[vmem, hbm],
        out_specs=hbm,
        scratch_shapes=[pltpu.SemaphoreType.DMA],
        input_output_aliases={1: 0},
        compiler_params=pltpu.CompilerParams(vmem_limit_bytes=4 * 1024 * 1024),
        name="complete",
    )(got, old)


def shards(n, tps, units, *args):
    w, low, high = args[0:12:3], [x.T for x in args[1:12:3]], args[2:12:3]
    norm_train, norm_step = args[12].reshape(1, -1), args[13].reshape(1, -1)
    kinds = len(w)
    by_column = [False] * (kinds - 1) + [True]
    stacked = [by_column[k] and w[k].shape[1] % 128 != 0 for k in range(kinds)]
    firsts = {order[0]: (128, 128), order[1]: (128,)}
    pieces = [pieces_of(w[k].shape[0], firsts.get(k, ())) for k in range(kinds)]
    count = sum(map(len, pieces))
    rounds = rounds_of(tps, 0)
    crossings = (len(rounds), max(map(len, rounds), default=0))
    shapes = []
    for k in range(kinds):
        rows, columns = w[k].shape
        if stacked[k]:
            shapes.append((n, rows, columns))
        elif by_column[k]:
            shapes.append((rows, n * columns))
        else:
            shapes.append((n * rows, columns))
    share = norm_train.shape[1]
    total = n * tps * share
    width = 128 if total % 128 == 0 else total
    vmem, hbm = pl.BlockSpec(memory_space=pltpu.VMEM), pl.BlockSpec(memory_space=pltpu.HBM)
    dma = pltpu.SemaphoreType.DMA
    operands = (*w, *low, *high, norm_train, norm_step)
    results = pl.pallas_call(
        functools.partial(kernel, n, tps, units, stacked, pieces),
        out_shape=[pltpu.VMEM(s, jnp.bfloat16) for s in shapes]
        + [pltpu.VMEM((total // width, width), jnp.bfloat16)],
        in_specs=[hbm] * (3 * kinds + 2),
        out_specs=[vmem] * (kinds + 1),
        scratch_shapes=[pltpu.VMEM(x.shape, x.dtype) for x in (*w, *low, *high)]
        + [pltpu.VMEM(x.shape[::-1], x.dtype) for x in low]
        + [
            pltpu.VMEM((2, 1, share), jnp.float32),
            pltpu.VMEM((n, tps, 1, share), jnp.float32),
            dma((2,)),
            dma((count,)),
            dma((2, kinds)),
            dma((2, count)),
            dma((2, count)),
            dma((n, kinds)),
            dma((n, kinds)),
            dma((2, n)),
            dma((n,)),
            dma(crossings),
            dma(crossings),
        ],
        compiler_params=pltpu.CompilerParams(
            collective_id=0, has_side_effects=True, vmem_limit_bytes=24 * 1024 * 1024
        ),
        name="merge_and_gather",
    )(*[pltpu.with_memory_space_constraint(x, pltpu.HBM) for x in operands])
    have = results[late_kind]
    *results, after = place(n, units, results)
    if n > 1:
        results[late_kind] = complete(n, units, finish(n, units, have, after), results[late_kind])
    finals = []
    for k in range(kinds):
        full = results[k]
        if stacked[k]:
            full = full.transpose(1, 0, 2).reshape(full.shape[1], -1)
        finals.append(full)
    return (*finals, results[kinds].reshape(-1))


def solution(mesh):
    return jax.shard_map(
        functools.partial(shards, mesh.shape["rows"], mesh.shape["tp"], mesh.shape["unit"]),
        mesh=mesh,
        in_specs=(
            P(("unit", "rows"), "tp"),
            P(("unit", "rows"), None),
            P("unit", "tp"),
            P(("unit", "rows"), "tp"),
            P(("unit", "rows"), None),
            P("unit", "tp"),
            P(("unit", "rows"), "tp"),
            P(("unit", "rows"), None),
            P("unit", "tp"),
            P(("unit", "tp"), "rows"),
            P(("unit", "tp"), None),
            P("unit", "rows"),
            P(("unit", "rows", "tp")),
            P(("unit", "rows", "tp")),
        ),
        out_specs=(
            P("unit", "tp"),
            P("unit", "tp"),
            P("unit", "tp"),
            P(("unit", "tp"), None),
            P("unit"),
        ),
        check_vma=False,
    )
```

```python
import functools

import jax
import jax.numpy as jnp
from jax import lax
from jax.experimental import pallas as pl
from jax.experimental.pallas import tpu as pltpu
from jax.sharding import PartitionSpec as P

MESH = pl.DeviceIdType.MESH
mix_rate = 0.5
order = (1, 0, 3, 2)
late_kind = order[-1]


def pieces_of(rows, firsts):
    sizes = [size for size in firsts if sum(firsts) < rows]
    left = rows - sum(sizes)
    return [*sizes, left] if left % 16 == 0 or not sizes else [rows]


def rounds_of(tps, t):
    if tps & (tps - 1):
        return [[(lax.rem(t + step, tps), t, lax.rem(t + tps - step, tps), 1) for step in range(1, tps)]]
    rounds, size = [], 1
    while size < tps:
        side = lax.rem(t // size, 2)
        base = (t // size) * size
        across = size - 2 * size * side
        rounds.append([(t + across, base, base + across, size)])
        size *= 2
    return rounds


def block_of(size, options):
    for option in options:
        if size % option == 0:
            return option
    return size


def kernel(n, tps, units, stacked, pieces, *refs):
    kinds = len(pieces)
    w, low, high = refs[:kinds], refs[kinds : 2 * kinds], refs[2 * kinds : 3 * kinds]
    norm_train, norm_step = refs[3 * kinds : 3 * kinds + 2]
    refs = refs[3 * kinds + 2 :]
    out, norm_out = refs[:kinds], refs[kinds]
    refs = refs[kinds + 1 :]
    w_own, low_own, high_own = refs[:kinds], refs[kinds : 2 * kinds], refs[2 * kinds : 3 * kinds]
    low_rows = refs[3 * kinds : 4 * kinds]
    refs = refs[4 * kinds :]
    norm_own, norm_all, norm_sem, load_sem, side_sem, send_sem, recv_sem, pass_send, pass_recv, norm_send, norm_recv, down_sem, cross_send, cross_recv = refs

    z, t = lax.axis_index("rows"), lax.axis_index("tp")
    late = lax.axis_index("unit") == units - 1
    rounds = rounds_of(tps, t)
    chunks = [(k, p) for k in order for p in range(len(pieces[k]))]
    has_up, has_down = z < n - 1, z > 0
    middle, top = n // 2, z == n - 1
    greeted = (has_up & (z >= middle), has_down & (z <= middle))
    waits = (has_up & ~greeted[0], has_down & ~greeted[1])
    held_up, held_down = late & (z == n - 2), late & (z == 1)
    missing_up, missing_down = late & (z == n - 1), late & (z == 0)

    def sends(k, direction):
        has, held = ((has_up, held_up), (has_down, held_down))[direction]
        return has & ~held if k == late_kind else has

    def comes(k, d, direction):
        has, missing = ((z - d >= 0, missing_up), (z + d < n, missing_down))[direction]
        return has & ~missing if k == late_kind else has

    def rows_of(k, p):
        return sum(pieces[k][:p]), pieces[k][p]

    def load(i):
        k, p = chunks[i]
        start, size = rows_of(k, p)
        return pltpu.make_async_copy(
            w[k].at[pl.ds(start, size)], w_own[k].at[pl.ds(start, size)], load_sem.at[i]
        )

    def side(k):
        return (
            pltpu.make_async_copy(low[k], low_own[k], side_sem.at[0, k]),
            pltpu.make_async_copy(high[k], high_own[k], side_sem.at[1, k]),
        )

    def load_kind(kind):
        for copy in side(kind):
            copy.start()
        for i, (k, p) in enumerate(chunks):
            if k == kind:
                load(i).start()

    barrier = pltpu.get_barrier_semaphore()

    @pl.when(z < middle)
    def _():
        pl.semaphore_signal(barrier, inc=1, device_id={"rows": z + 1}, device_id_type=MESH)

    @pl.when(z > middle)
    def _():
        pl.semaphore_signal(barrier, inc=1, device_id={"rows": z - 1}, device_id_type=MESH)

    @pl.when(top)
    def _():
        for partner in [exchange[0] for exchanges in rounds for exchange in exchanges]:
            pl.semaphore_signal(barrier, inc=1, device_id={"tp": partner}, device_id_type=MESH)

    for kind in order:
        load_kind(kind)

    norm_loads = [
        pltpu.make_async_copy(source, norm_own.at[j], norm_sem.at[j])
        for j, source in enumerate((norm_train, norm_step))
    ]
    for copy in norm_loads:
        copy.start()

    def region(k, p, origin):
        start, size = (0, w[k].shape[0]) if p is None else rows_of(k, p)
        columns = w[k].shape[1]
        if stacked[k]:
            return out[k].at[origin, pl.ds(start, size)]
        if out[k].shape[1] == columns:
            rows = w[k].shape[0]
            return out[k].at[pl.ds(pl.multiple_of(origin * rows + start, 16), size)]
        return out[k].at[pl.ds(start, size), pl.ds(pl.multiple_of(origin * columns, 128), columns)]

    def hop(place, send, recv, direction):
        return pltpu.make_async_remote_copy(
            src_ref=place,
            dst_ref=place,
            send_sem=send,
            recv_sem=recv,
            device_id={"rows": z + 1 - 2 * direction},
            device_id_type=MESH,
        )

    def chunk_hop(i, origin, direction):
        k, p = chunks[i]
        return hop(region(k, p, origin), send_sem.at[direction, i], recv_sem.at[direction, i], direction)

    def whole_hop(k, origin, direction):
        return hop(
            region(k, None, origin),
            pass_send.at[origin, k],
            pass_recv.at[origin, k],
            direction,
        )

    def norm_hop(origin):
        return pltpu.make_async_remote_copy(
            src_ref=norm_all.at[origin, t],
            dst_ref=norm_all.at[origin, t],
            send_sem=norm_send.at[origin],
            recv_sem=norm_recv.at[origin],
            device_id={"rows": z + 1},
            device_id_type=MESH,
        )

    def norm_down():
        return pltpu.make_async_remote_copy(
            src_ref=norm_out,
            dst_ref=norm_out,
            send_sem=down_sem.at[0],
            recv_sem=down_sem.at[1],
            device_id={"rows": z - 1},
            device_id_type=MESH,
        )

    def cross(r, j, coming=False):
        partner, base, theirs, size = rounds[r][j]
        place = norm_all.at[:, pl.ds(theirs if coming else base, size)]
        return pltpu.make_async_remote_copy(
            src_ref=place,
            dst_ref=place,
            send_sem=cross_send.at[r, j],
            recv_sem=cross_recv.at[r, j],
            device_id={"tp": partner},
            device_id_type=MESH,
        )

    def cross_start(r):
        for j in range(len(rounds[r])):
            cross(r, j).start()

    def cross_wait(r):
        for j in range(len(rounds[r])):
            cross(r, j, coming=True).wait_recv()

    def send_greeted(i):
        for direction in range(2):

            @pl.when(sends(chunks[i][0], direction) & greeted[direction])
            def _():
                chunk_hop(i, z, direction).start()

    def send_late():
        for direction in range(2):

            @pl.when(waits[direction])
            def _():
                chunk_hop(0, z + 1 - 2 * direction, 1 - direction).wait_recv()
                if direction == 0:
                    norm_hop(z).start()
                for i, (k, _) in enumerate(chunks):

                    @pl.when(sends(k, direction))
                    def _():
                        chunk_hop(i, z, direction).start()

    def merge(i):
        k, p = chunks[i]
        start, size = rows_of(k, p)
        columns = w[k].shape[1]
        high_block = block_of(size, (160, 128, 64, 32, 16))
        wide_block = block_of(columns, (256, 128))
        wides = columns // wide_block
        place = region(k, p, z)

        def body(b, _):
            if size == high_block:
                r, c = 0, b
            else:
                r, c = b // wides, b % wides
            r = r * high_block
            c = 0 if wides == 1 else pl.multiple_of(c * wide_block, wide_block)
            mine = pl.ds(start + r, high_block)
            wide = pl.ds(c, wide_block)
            result = w_own[k][mine, wide].astype(jnp.float32) + mix_rate * jnp.dot(
                low_rows[k][mine, :], high_own[k][:, wide], preferred_element_type=jnp.float32
            )
            place[pl.ds(r, high_block), wide] = result.astype(jnp.bfloat16)
            return 0

        lax.fori_loop(0, (size // high_block) * wides, body, 0)

    for i, (k, p) in enumerate(chunks):
        if p == 0:
            for copy in side(k):
                copy.wait()
        mine = pl.ds(*rows_of(k, p))
        low_rows[k][mine, :] = low_own[k][:, mine].astype(jnp.float32).T.astype(jnp.bfloat16)
        if i == 1:
            partners = greeted[0].astype(jnp.int32) + greeted[1].astype(jnp.int32)
            partners += top.astype(jnp.int32) * sum(map(len, rounds))

            @pl.when(partners > 0)
            def _():
                pl.semaphore_wait(barrier, partners)

        if i > 0:
            send_greeted(i - 1)
        load(i).wait()
        merge(i)
        if i == min(3, len(chunks) - 2):
            for copy in norm_loads:
                copy.wait()
            norm_all[z, t] = (norm_own[0] + norm_own[1]).astype(jnp.bfloat16).astype(jnp.float32)
        if i == min(4, len(chunks) - 1):

            @pl.when(greeted[0])
            def _():
                norm_hop(z).start()

    send_greeted(len(chunks) - 1)
    send_late()

    def arrival(arrived, onward, d, k, near):
        for direction, origin in ((0, z - d), (1, z + d)):

            @pl.when(comes(k, d, direction))
            def _():
                for j, make in enumerate(arrived):
                    if near and k == order[0] and j == 0:

                        @pl.when(~waits[1 - direction])
                        def _():
                            make(origin, direction).wait_recv()

                    else:
                        make(origin, direction).wait_recv()

                @pl.when(sends(k, direction))
                def _():
                    onward(origin, direction).start()

    def distance(d, _, near=False):
        @pl.when(z - d >= 0)
        def _():
            norm_hop(z - d).wait_recv()

            @pl.when(has_up)
            def _():
                norm_hop(z - d).start()

        for j, k in enumerate(order):

            @pl.when(top & (d == n - 1))
            def _():
                if j == 0:
                    share_norm()
                if j == 1:
                    norm_down().start()

            onward = functools.partial(whole_hop, k)
            arrived = [onward]
            if near:
                arrived = [functools.partial(chunk_hop, i) for i, c in enumerate(chunks) if c[0] == k]
            arrival(arrived, onward, d, k, near)
        return 0

    def share_norm():
        for r in range(len(rounds)):
            cross_start(r)
            cross_wait(r)
        write_norm()

    def write_norm():
        line = jnp.concatenate([norm_all[a, b] for a in range(n) for b in range(tps)], axis=1)
        width = norm_out.shape[1]
        norm_out[...] = jnp.concatenate(
            [line[:, a * width : (a + 1) * width] for a in range(norm_out.shape[0])], axis=0
        ).astype(jnp.bfloat16)

    distance(jnp.int32(1), 0, near=True)
    lax.fori_loop(2, n, distance, 0)

    @pl.when(has_up)
    def _():
        norm_down().wait_recv()

    @pl.when(has_up & has_down)
    def _():
        norm_down().start()

    for direction in range(2):
        for i in range(len(chunks)):

            @pl.when(sends(chunks[i][0], direction))
            def _():
                chunk_hop(i, z, direction).wait_send()

    @pl.when(has_up)
    def _():
        norm_hop(z).wait_send()

    @pl.when(has_down)
    def _():
        norm_down().wait_send()

    def drain(origin, _):
        for direction, passed in ((0, origin < z), (1, origin > z)):
            for k in range(kinds):

                @pl.when(sends(k, direction) & passed)
                def _():
                    whole_hop(k, origin, direction).wait_send()

        @pl.when(has_up & (origin < z))
        def _():
            norm_hop(origin).wait_send()

        return 0

    lax.fori_loop(0, n, drain, 0)

    @pl.when(top)
    def _():
        for r in range(len(rounds)):
            for j in range(len(rounds[r])):
                cross(r, j).wait_send()


def ends(n, units):
    z, late = lax.axis_index("rows"), lax.axis_index("unit") == units - 1
    return late & (z == 0), late & (z == n - 1)


def put(n, units, parts, *refs):
    kinds = len(parts)
    src, dst, sem = refs[:kinds], refs[kinds : 2 * kinds], refs[-1]
    bottom, top = ends(n, units)
    copies, kept = [], []
    for k in range(kinds):
        size = src[k].shape[0] // parts[k]
        for p in range(parts[k]):
            rows = pl.ds(p * size, size)
            copy = pltpu.make_async_copy(src[k].at[rows], dst[k].at[rows], sem.at[len(copies) + len(kept)])
            (kept if k == late_kind else copies).append(copy)
    share = src[late_kind].shape[0] // n

    def own(origin):
        rows = pl.ds(origin * share, share)
        return pltpu.make_async_copy(src[late_kind].at[rows], dst[late_kind].at[rows], sem.at[sum(parts)])

    for copy in copies:
        copy.start()

    @pl.when(~bottom & ~top)
    def _():
        for copy in kept:
            copy.start()
        for copy in kept:
            copy.wait()

    for flag, origin in ((bottom, 0), (top, n - 1)):

        @pl.when(flag)
        def _():
            own(origin).start()
            own(origin).wait()

    for copy in copies:
        copy.wait()


def place(n, units, arrays):
    parts = [2 if x.shape[0] % 128 == 0 else 1 for x in arrays]
    vmem, hbm = pl.BlockSpec(memory_space=pltpu.VMEM), pl.BlockSpec(memory_space=pltpu.HBM)
    return pl.pallas_call(
        functools.partial(put, n, units, parts),
        out_shape=[pltpu.HBM(x.shape, x.dtype) for x in arrays] + [pltpu.VMEM((8, 128), jnp.float32)],
        in_specs=[vmem] * len(arrays),
        out_specs=[hbm] * len(arrays) + [vmem],
        scratch_shapes=[pltpu.SemaphoreType.DMA((sum(parts) + 1,))],
        compiler_params=pltpu.CompilerParams(vmem_limit_bytes=24 * 1024 * 1024),
        name="place",
    )(*arrays)


def last_hop(n, units, have, after, got, send_sem, recv_sem):
    z, late = lax.axis_index("rows"), lax.axis_index("unit") == units - 1
    bottom, top = ends(n, units)
    size = got.shape[0]
    share = have.shape[0] - size

    def hop(direction):
        return pltpu.make_async_remote_copy(
            src_ref=have.at[pl.ds(share * direction, size)],
            dst_ref=got,
            send_sem=send_sem.at[direction],
            recv_sem=recv_sem.at[direction],
            device_id={"rows": z + 1 - 2 * direction},
            device_id_type=MESH,
        )

    barrier = pltpu.get_barrier_semaphore()
    above, below = late & (z == n - 2), late & (z == 1)

    @pl.when(bottom)
    def _():
        pl.semaphore_signal(barrier, inc=1, device_id={"rows": z + 1}, device_id_type=MESH)

    @pl.when(top)
    def _():
        pl.semaphore_signal(barrier, inc=1, device_id={"rows": z - 1}, device_id_type=MESH)

    @pl.when(above | below)
    def _():
        pl.semaphore_wait(barrier, above.astype(jnp.int32) + below.astype(jnp.int32))

    for direction, flag in ((0, above), (1, below)):

        @pl.when(flag)
        def _():
            hop(direction).start()

    for direction, flag in ((0, top), (1, bottom)):

        @pl.when(flag)
        def _():
            hop(direction).wait_recv()

    for direction, flag in ((0, above), (1, below)):

        @pl.when(flag)
        def _():
            hop(direction).wait_send()


def finish(n, units, have, after):
    share = have.shape[0] // n
    vmem, dma = pl.BlockSpec(memory_space=pltpu.VMEM), pltpu.SemaphoreType.DMA
    return pl.pallas_call(
        functools.partial(last_hop, n, units),
        out_shape=pltpu.VMEM((have.shape[0] - share, have.shape[1]), have.dtype),
        in_specs=[vmem, vmem],
        out_specs=vmem,
        scratch_shapes=[dma((2,)), dma((2,))],
        compiler_params=pltpu.CompilerParams(
            collective_id=1, has_side_effects=True, vmem_limit_bytes=4 * 1024 * 1024
        ),
        name="last_hop",
    )(have, after)


def add_rows(n, units, got, old, out, sem):
    size = got.shape[0]
    share = out.shape[0] - size
    for flag, start in zip(ends(n, units), (share, 0)):

        @pl.when(flag)
        def _():
            copy = pltpu.make_async_copy(got, out.at[pl.ds(start, size)], sem)
            copy.start()
            copy.wait()


def complete(n, units, got, old):
    vmem, hbm = pl.BlockSpec(memory_space=pltpu.VMEM), pl.BlockSpec(memory_space=pltpu.HBM)
    return pl.pallas_call(
        functools.partial(add_rows, n, units),
        out_shape=pltpu.HBM(old.shape, old.dtype),
        in_specs=[vmem, hbm],
        out_specs=hbm,
        scratch_shapes=[pltpu.SemaphoreType.DMA],
        input_output_aliases={1: 0},
        compiler_params=pltpu.CompilerParams(vmem_limit_bytes=4 * 1024 * 1024),
        name="complete",
    )(got, old)


def shards(n, tps, units, *args):
    w, low, high = args[0:12:3], [x.T for x in args[1:12:3]], args[2:12:3]
    norm_train, norm_step = args[12].reshape(1, -1), args[13].reshape(1, -1)
    kinds = len(w)
    by_column = [False] * (kinds - 1) + [True]
    stacked = [by_column[k] and w[k].shape[1] % 128 != 0 for k in range(kinds)]
    firsts = {order[0]: (128, 128), order[1]: (128,)}
    pieces = [pieces_of(w[k].shape[0], firsts.get(k, ())) for k in range(kinds)]
    count = sum(map(len, pieces))
    rounds = rounds_of(tps, 0)
    crossings = (len(rounds), max(map(len, rounds), default=0))
    shapes = []
    for k in range(kinds):
        rows, columns = w[k].shape
        if stacked[k]:
            shapes.append((n, rows, columns))
        elif by_column[k]:
            shapes.append((rows, n * columns))
        else:
            shapes.append((n * rows, columns))
    share = norm_train.shape[1]
    total = n * tps * share
    width = 128 if total % 128 == 0 else total
    vmem, hbm = pl.BlockSpec(memory_space=pltpu.VMEM), pl.BlockSpec(memory_space=pltpu.HBM)
    dma = pltpu.SemaphoreType.DMA
    operands = (*w, *low, *high, norm_train, norm_step)
    results = pl.pallas_call(
        functools.partial(kernel, n, tps, units, stacked, pieces),
        out_shape=[pltpu.VMEM(s, jnp.bfloat16) for s in shapes]
        + [pltpu.VMEM((total // width, width), jnp.bfloat16)],
        in_specs=[hbm] * (3 * kinds + 2),
        out_specs=[vmem] * (kinds + 1),
        scratch_shapes=[pltpu.VMEM(x.shape, x.dtype) for x in (*w, *low, *high)]
        + [pltpu.VMEM(x.shape[::-1], x.dtype) for x in low]
        + [
            pltpu.VMEM((2, 1, share), jnp.float32),
            pltpu.VMEM((n, tps, 1, share), jnp.float32),
            dma((2,)),
            dma((count,)),
            dma((2, kinds)),
            dma((2, count)),
            dma((2, count)),
            dma((n, kinds)),
            dma((n, kinds)),
            dma((n,)),
            dma((n,)),
            dma((2,)),
            dma(crossings),
            dma(crossings),
        ],
        compiler_params=pltpu.CompilerParams(
            collective_id=0, has_side_effects=True, vmem_limit_bytes=24 * 1024 * 1024
        ),
        name="merge_and_gather",
    )(*[pltpu.with_memory_space_constraint(x, pltpu.HBM) for x in operands])
    have = results[late_kind]
    *results, after = place(n, units, results)
    if n > 1:
        results[late_kind] = complete(n, units, finish(n, units, have, after), results[late_kind])
    finals = []
    for k in range(kinds):
        full = results[k]
        if stacked[k]:
            full = full.transpose(1, 0, 2).reshape(full.shape[1], -1)
        finals.append(full)
    return (*finals, results[kinds].reshape(-1))


def solution(mesh):
    return jax.shard_map(
        functools.partial(shards, mesh.shape["rows"], mesh.shape["tp"], mesh.shape["unit"]),
        mesh=mesh,
        in_specs=(
            P(("unit", "rows"), "tp"),
            P(("unit", "rows"), None),
            P("unit", "tp"),
            P(("unit", "rows"), "tp"),
            P(("unit", "rows"), None),
            P("unit", "tp"),
            P(("unit", "rows"), "tp"),
            P(("unit", "rows"), None),
            P("unit", "tp"),
            P(("unit", "tp"), "rows"),
            P(("unit", "tp"), None),
            P("unit", "rows"),
            P(("unit", "rows", "tp")),
            P(("unit", "rows", "tp")),
        ),
        out_specs=(
            P("unit", "tp"),
            P("unit", "tp"),
            P("unit", "tp"),
            P(("unit", "tp"), None),
            P("unit"),
        ),
        check_vma=False,
    )
```

```python
import functools

import jax
import jax.numpy as jnp
from jax import lax
from jax.experimental import pallas as pl
from jax.experimental.pallas import tpu as pltpu
from jax.sharding import PartitionSpec as P

MESH = pl.DeviceIdType.MESH
mix_rate = 0.5
order = (1, 0, 3, 2)
late_kind = order[-1]


def pieces_of(rows, firsts):
    sizes = [size for size in firsts if sum(firsts) < rows]
    left = rows - sum(sizes)
    return [*sizes, left] if left % 16 == 0 or not sizes else [rows]


def rounds_of(tps, t):
    if tps & (tps - 1):
        return [[(lax.rem(t + step, tps), t, lax.rem(t + tps - step, tps), 1) for step in range(1, tps)]]
    rounds, size = [], 1
    while size < tps:
        side = lax.rem(t // size, 2)
        base = (t // size) * size
        across = size - 2 * size * side
        rounds.append([(t + across, base, base + across, size)])
        size *= 2
    return rounds


def block_of(size, options):
    for option in options:
        if size % option == 0:
            return option
    return size


def kernel(n, tps, units, stacked, pieces, *refs):
    kinds = len(pieces)
    w, low, high = refs[:kinds], refs[kinds : 2 * kinds], refs[2 * kinds : 3 * kinds]
    norm_train, norm_step = refs[3 * kinds : 3 * kinds + 2]
    refs = refs[3 * kinds + 2 :]
    out, norm_out = refs[:kinds], refs[kinds]
    refs = refs[kinds + 1 :]
    w_own, low_own, high_own = refs[:kinds], refs[kinds : 2 * kinds], refs[2 * kinds : 3 * kinds]
    low_rows = refs[3 * kinds : 4 * kinds]
    refs = refs[4 * kinds :]
    norm_own, norm_all, norm_sem, load_sem, side_sem, send_sem, recv_sem, pass_send, pass_recv, norm_send, norm_recv, down_sem, cross_send, cross_recv = refs

    z, t = lax.axis_index("rows"), lax.axis_index("tp")
    late = lax.axis_index("unit") == units - 1
    rounds = rounds_of(tps, t)
    chunks = [(k, p) for k in order for p in range(len(pieces[k]))]
    has_up, has_down = z < n - 1, z > 0
    middle, top = n // 2, z == n - 1
    greeted = (has_up & (z >= middle), has_down & (z <= middle))
    waits = (has_up & ~greeted[0], has_down & ~greeted[1])
    held_up, held_down = late & (z == n - 2), late & (z == 1)
    missing_up, missing_down = late & (z == n - 1), late & (z == 0)

    def sends(k, direction):
        has, held = ((has_up, held_up), (has_down, held_down))[direction]
        return has & ~held if k == late_kind else has

    def comes(k, d, direction):
        has, missing = ((z - d >= 0, missing_up), (z + d < n, missing_down))[direction]
        return has & ~missing if k == late_kind else has

    def rows_of(k, p):
        return sum(pieces[k][:p]), pieces[k][p]

    def load(i):
        k, p = chunks[i]
        start, size = rows_of(k, p)
        return pltpu.make_async_copy(
            w[k].at[pl.ds(start, size)], w_own[k].at[pl.ds(start, size)], load_sem.at[i]
        )

    def side(k):
        return (
            pltpu.make_async_copy(low[k], low_own[k], side_sem.at[0, k]),
            pltpu.make_async_copy(high[k], high_own[k], side_sem.at[1, k]),
        )

    def load_kind(kind):
        for copy in side(kind):
            copy.start()
        for i, (k, p) in enumerate(chunks):
            if k == kind:
                load(i).start()

    barrier = pltpu.get_barrier_semaphore()

    @pl.when(z < middle)
    def _():
        pl.semaphore_signal(barrier, inc=1, device_id={"rows": z + 1}, device_id_type=MESH)

    @pl.when(z > middle)
    def _():
        pl.semaphore_signal(barrier, inc=1, device_id={"rows": z - 1}, device_id_type=MESH)

    @pl.when(top)
    def _():
        for partner in [exchange[0] for exchanges in rounds for exchange in exchanges]:
            pl.semaphore_signal(barrier, inc=1, device_id={"tp": partner}, device_id_type=MESH)

    for kind in order:
        load_kind(kind)

    norm_loads = [
        pltpu.make_async_copy(source, norm_own.at[j], norm_sem.at[j])
        for j, source in enumerate((norm_train, norm_step))
    ]
    for copy in norm_loads:
        copy.start()

    def region(k, p, origin):
        start, size = (0, w[k].shape[0]) if p is None else rows_of(k, p)
        columns = w[k].shape[1]
        if stacked[k]:
            return out[k].at[origin, pl.ds(start, size)]
        if out[k].shape[1] == columns:
            rows = w[k].shape[0]
            return out[k].at[pl.ds(pl.multiple_of(origin * rows + start, 16), size)]
        return out[k].at[pl.ds(start, size), pl.ds(pl.multiple_of(origin * columns, 128), columns)]

    def hop(place, send, recv, direction):
        return pltpu.make_async_remote_copy(
            src_ref=place,
            dst_ref=place,
            send_sem=send,
            recv_sem=recv,
            device_id={"rows": z + 1 - 2 * direction},
            device_id_type=MESH,
        )

    def chunk_hop(i, origin, direction):
        k, p = chunks[i]
        return hop(region(k, p, origin), send_sem.at[direction, i], recv_sem.at[direction, i], direction)

    def whole_hop(k, origin, direction):
        return hop(
            region(k, None, origin),
            pass_send.at[origin, k],
            pass_recv.at[origin, k],
            direction,
        )

    def norm_hop(origin):
        return pltpu.make_async_remote_copy(
            src_ref=norm_all.at[origin, t],
            dst_ref=norm_all.at[origin, t],
            send_sem=norm_send.at[origin],
            recv_sem=norm_recv.at[origin],
            device_id={"rows": z + 1},
            device_id_type=MESH,
        )

    def norm_down():
        return pltpu.make_async_remote_copy(
            src_ref=norm_out,
            dst_ref=norm_out,
            send_sem=down_sem.at[0],
            recv_sem=down_sem.at[1],
            device_id={"rows": z - 1},
            device_id_type=MESH,
        )

    def cross(r, j, coming=False):
        partner, base, theirs, size = rounds[r][j]
        place = norm_all.at[:, pl.ds(theirs if coming else base, size)]
        return pltpu.make_async_remote_copy(
            src_ref=place,
            dst_ref=place,
            send_sem=cross_send.at[r, j],
            recv_sem=cross_recv.at[r, j],
            device_id={"tp": partner},
            device_id_type=MESH,
        )

    def cross_start(r):
        for j in range(len(rounds[r])):
            cross(r, j).start()

    def cross_wait(r):
        for j in range(len(rounds[r])):
            cross(r, j, coming=True).wait_recv()

    def send_greeted(i):
        for direction in range(2):

            @pl.when(sends(chunks[i][0], direction) & greeted[direction])
            def _():
                chunk_hop(i, z, direction).start()

    def send_late():
        for direction in range(2):

            @pl.when(waits[direction])
            def _():
                chunk_hop(0, z + 1 - 2 * direction, 1 - direction).wait_recv()
                if direction == 0:
                    norm_hop(z).start()
                for i, (k, _) in enumerate(chunks):

                    @pl.when(sends(k, direction))
                    def _():
                        chunk_hop(i, z, direction).start()

    def merge(i):
        k, p = chunks[i]
        start, size = rows_of(k, p)
        columns = w[k].shape[1]
        high_block = block_of(size, (160, 128, 64, 32, 16))
        wide_block = block_of(columns, (256, 128))
        wides = columns // wide_block
        place = region(k, p, z)

        def body(b, _):
            if size == high_block:
                r, c = 0, b
            else:
                r, c = b // wides, b % wides
            r = r * high_block
            c = 0 if wides == 1 else pl.multiple_of(c * wide_block, wide_block)
            mine = pl.ds(start + r, high_block)
            wide = pl.ds(c, wide_block)
            result = w_own[k][mine, wide].astype(jnp.float32) + mix_rate * jnp.dot(
                low_rows[k][mine, :], high_own[k][:, wide], preferred_element_type=jnp.float32
            )
            place[pl.ds(r, high_block), wide] = result.astype(jnp.bfloat16)
            return 0

        lax.fori_loop(0, (size // high_block) * wides, body, 0)

    for i, (k, p) in enumerate(chunks):
        if p == 0:
            for copy in side(k):
                copy.wait()
        mine = pl.ds(*rows_of(k, p))
        low_rows[k][mine, :] = low_own[k][:, mine].astype(jnp.float32).T.astype(jnp.bfloat16)
        load(i).wait()
        merge(i)
        if i == 1:
            partners = greeted[0].astype(jnp.int32) + greeted[1].astype(jnp.int32)
            partners += top.astype(jnp.int32) * sum(map(len, rounds))

            @pl.when(partners > 0)
            def _():
                pl.semaphore_wait(barrier, partners)

        if i > 0:
            send_greeted(i - 1)
        if i == min(3, len(chunks) - 2):
            for copy in norm_loads:
                copy.wait()
            norm_all[z, t] = (norm_own[0] + norm_own[1]).astype(jnp.bfloat16).astype(jnp.float32)
        if i == min(4, len(chunks) - 1):

            @pl.when(greeted[0])
            def _():
                norm_hop(z).start()

    send_greeted(len(chunks) - 1)
    send_late()

    def arrival(arrived, onward, d, k, near):
        for direction, origin in ((0, z - d), (1, z + d)):

            @pl.when(comes(k, d, direction))
            def _():
                for j, make in enumerate(arrived):
                    if near and k == order[0] and j == 0:

                        @pl.when(~waits[1 - direction])
                        def _():
                            make(origin, direction).wait_recv()

                    else:
                        make(origin, direction).wait_recv()

                @pl.when(sends(k, direction))
                def _():
                    onward(origin, direction).start()

    def distance(d, _, near=False):
        @pl.when(z - d >= 0)
        def _():
            norm_hop(z - d).wait_recv()

            @pl.when(has_up)
            def _():
                norm_hop(z - d).start()

        for j, k in enumerate(order):

            @pl.when(top & (d == n - 1))
            def _():
                if j == 0:
                    share_norm()
                if j == 1:
                    norm_down().start()

            onward = functools.partial(whole_hop, k)
            arrived = [onward]
            if near:
                arrived = [functools.partial(chunk_hop, i) for i, c in enumerate(chunks) if c[0] == k]
            arrival(arrived, onward, d, k, near)
        return 0

    def share_norm():
        for r in range(len(rounds)):
            cross_start(r)
            cross_wait(r)
        write_norm()

    def write_norm():
        line = jnp.concatenate([norm_all[a, b] for a in range(n) for b in range(tps)], axis=1)
        width = norm_out.shape[1]
        norm_out[...] = jnp.concatenate(
            [line[:, a * width : (a + 1) * width] for a in range(norm_out.shape[0])], axis=0
        ).astype(jnp.bfloat16)

    distance(jnp.int32(1), 0, near=True)
    lax.fori_loop(2, n, distance, 0)

    @pl.when(has_up)
    def _():
        norm_down().wait_recv()

    @pl.when(has_up & has_down)
    def _():
        norm_down().start()

    for direction in range(2):
        for i in range(len(chunks)):

            @pl.when(sends(chunks[i][0], direction))
            def _():
                chunk_hop(i, z, direction).wait_send()

    @pl.when(has_up)
    def _():
        norm_hop(z).wait_send()

    @pl.when(has_down)
    def _():
        norm_down().wait_send()

    def drain(origin, _):
        for direction, passed in ((0, origin < z), (1, origin > z)):
            for k in range(kinds):

                @pl.when(sends(k, direction) & passed)
                def _():
                    whole_hop(k, origin, direction).wait_send()

        @pl.when(has_up & (origin < z))
        def _():
            norm_hop(origin).wait_send()

        return 0

    lax.fori_loop(0, n, drain, 0)

    @pl.when(top)
    def _():
        for r in range(len(rounds)):
            for j in range(len(rounds[r])):
                cross(r, j).wait_send()


def ends(n, units):
    z, late = lax.axis_index("rows"), lax.axis_index("unit") == units - 1
    return late & (z == 0), late & (z == n - 1)


def put(n, units, parts, *refs):
    kinds = len(parts)
    src, dst, sem = refs[:kinds], refs[kinds : 2 * kinds], refs[-1]
    bottom, top = ends(n, units)
    copies, kept = [], []
    for k in range(kinds):
        size = src[k].shape[0] // parts[k]
        for p in range(parts[k]):
            rows = pl.ds(p * size, size)
            copy = pltpu.make_async_copy(src[k].at[rows], dst[k].at[rows], sem.at[len(copies) + len(kept)])
            (kept if k == late_kind else copies).append(copy)
    share = src[late_kind].shape[0] // n

    def own(origin):
        rows = pl.ds(origin * share, share)
        return pltpu.make_async_copy(src[late_kind].at[rows], dst[late_kind].at[rows], sem.at[sum(parts)])

    for copy in copies:
        copy.start()

    @pl.when(~bottom & ~top)
    def _():
        for copy in kept:
            copy.start()
        for copy in kept:
            copy.wait()

    for flag, origin in ((bottom, 0), (top, n - 1)):

        @pl.when(flag)
        def _():
            own(origin).start()
            own(origin).wait()

    for copy in copies:
        copy.wait()


def place(n, units, arrays):
    parts = [2 if x.shape[0] % 128 == 0 else 1 for x in arrays]
    vmem, hbm = pl.BlockSpec(memory_space=pltpu.VMEM), pl.BlockSpec(memory_space=pltpu.HBM)
    return pl.pallas_call(
        functools.partial(put, n, units, parts),
        out_shape=[pltpu.HBM(x.shape, x.dtype) for x in arrays] + [pltpu.VMEM((8, 128), jnp.float32)],
        in_specs=[vmem] * len(arrays),
        out_specs=[hbm] * len(arrays) + [vmem],
        scratch_shapes=[pltpu.SemaphoreType.DMA((sum(parts) + 1,))],
        compiler_params=pltpu.CompilerParams(vmem_limit_bytes=24 * 1024 * 1024),
        name="place",
    )(*arrays)


def last_hop(n, units, have, after, got, send_sem, recv_sem):
    z, late = lax.axis_index("rows"), lax.axis_index("unit") == units - 1
    bottom, top = ends(n, units)
    size = got.shape[0]
    share = have.shape[0] - size

    def hop(direction):
        return pltpu.make_async_remote_copy(
            src_ref=have.at[pl.ds(share * direction, size)],
            dst_ref=got,
            send_sem=send_sem.at[direction],
            recv_sem=recv_sem.at[direction],
            device_id={"rows": z + 1 - 2 * direction},
            device_id_type=MESH,
        )

    barrier = pltpu.get_barrier_semaphore()
    above, below = late & (z == n - 2), late & (z == 1)

    @pl.when(bottom)
    def _():
        pl.semaphore_signal(barrier, inc=1, device_id={"rows": z + 1}, device_id_type=MESH)

    @pl.when(top)
    def _():
        pl.semaphore_signal(barrier, inc=1, device_id={"rows": z - 1}, device_id_type=MESH)

    @pl.when(above | below)
    def _():
        pl.semaphore_wait(barrier, above.astype(jnp.int32) + below.astype(jnp.int32))

    for direction, flag in ((0, above), (1, below)):

        @pl.when(flag)
        def _():
            hop(direction).start()

    for direction, flag in ((0, top), (1, bottom)):

        @pl.when(flag)
        def _():
            hop(direction).wait_recv()

    for direction, flag in ((0, above), (1, below)):

        @pl.when(flag)
        def _():
            hop(direction).wait_send()


def finish(n, units, have, after):
    share = have.shape[0] // n
    vmem, dma = pl.BlockSpec(memory_space=pltpu.VMEM), pltpu.SemaphoreType.DMA
    return pl.pallas_call(
        functools.partial(last_hop, n, units),
        out_shape=pltpu.VMEM((have.shape[0] - share, have.shape[1]), have.dtype),
        in_specs=[vmem, vmem],
        out_specs=vmem,
        scratch_shapes=[dma((2,)), dma((2,))],
        compiler_params=pltpu.CompilerParams(
            collective_id=1, has_side_effects=True, vmem_limit_bytes=4 * 1024 * 1024
        ),
        name="last_hop",
    )(have, after)


def add_rows(n, units, got, old, out, sem):
    size = got.shape[0]
    share = out.shape[0] - size
    for flag, start in zip(ends(n, units), (share, 0)):

        @pl.when(flag)
        def _():
            copy = pltpu.make_async_copy(got, out.at[pl.ds(start, size)], sem)
            copy.start()
            copy.wait()


def complete(n, units, got, old):
    vmem, hbm = pl.BlockSpec(memory_space=pltpu.VMEM), pl.BlockSpec(memory_space=pltpu.HBM)
    return pl.pallas_call(
        functools.partial(add_rows, n, units),
        out_shape=pltpu.HBM(old.shape, old.dtype),
        in_specs=[vmem, hbm],
        out_specs=hbm,
        scratch_shapes=[pltpu.SemaphoreType.DMA],
        input_output_aliases={1: 0},
        compiler_params=pltpu.CompilerParams(vmem_limit_bytes=4 * 1024 * 1024),
        name="complete",
    )(got, old)


def shards(n, tps, units, *args):
    w, low, high = args[0:12:3], [x.T for x in args[1:12:3]], args[2:12:3]
    norm_train, norm_step = args[12].reshape(1, -1), args[13].reshape(1, -1)
    kinds = len(w)
    by_column = [False] * (kinds - 1) + [True]
    stacked = [by_column[k] and w[k].shape[1] % 128 != 0 for k in range(kinds)]
    firsts = {order[0]: (128, 128), order[1]: (256,)}
    pieces = [pieces_of(w[k].shape[0], firsts.get(k, ())) for k in range(kinds)]
    count = sum(map(len, pieces))
    rounds = rounds_of(tps, 0)
    crossings = (len(rounds), max(map(len, rounds), default=0))
    shapes = []
    for k in range(kinds):
        rows, columns = w[k].shape
        if stacked[k]:
            shapes.append((n, rows, columns))
        elif by_column[k]:
            shapes.append((rows, n * columns))
        else:
            shapes.append((n * rows, columns))
    share = norm_train.shape[1]
    total = n * tps * share
    width = 128 if total % 128 == 0 else total
    vmem, hbm = pl.BlockSpec(memory_space=pltpu.VMEM), pl.BlockSpec(memory_space=pltpu.HBM)
    dma = pltpu.SemaphoreType.DMA
    operands = (*w, *low, *high, norm_train, norm_step)
    results = pl.pallas_call(
        functools.partial(kernel, n, tps, units, stacked, pieces),
        out_shape=[pltpu.VMEM(s, jnp.bfloat16) for s in shapes]
        + [pltpu.VMEM((total // width, width), jnp.bfloat16)],
        in_specs=[hbm] * (3 * kinds + 2),
        out_specs=[vmem] * (kinds + 1),
        scratch_shapes=[pltpu.VMEM(x.shape, x.dtype) for x in (*w, *low, *high)]
        + [pltpu.VMEM(x.shape[::-1], x.dtype) for x in low]
        + [
            pltpu.VMEM((2, 1, share), jnp.float32),
            pltpu.VMEM((n, tps, 1, share), jnp.float32),
            dma((2,)),
            dma((count,)),
            dma((2, kinds)),
            dma((2, count)),
            dma((2, count)),
            dma((n, kinds)),
            dma((n, kinds)),
            dma((n,)),
            dma((n,)),
            dma((2,)),
            dma(crossings),
            dma(crossings),
        ],
        compiler_params=pltpu.CompilerParams(
            collective_id=0, has_side_effects=True, vmem_limit_bytes=24 * 1024 * 1024
        ),
        name="merge_and_gather",
    )(*[pltpu.with_memory_space_constraint(x, pltpu.HBM) for x in operands])
    have = results[late_kind]
    *results, after = place(n, units, results)
    if n > 1:
        results[late_kind] = complete(n, units, finish(n, units, have, after), results[late_kind])
    finals = []
    for k in range(kinds):
        full = results[k]
        if stacked[k]:
            full = full.transpose(1, 0, 2).reshape(full.shape[1], -1)
        finals.append(full)
    return (*finals, results[kinds].reshape(-1))


def solution(mesh):
    return jax.shard_map(
        functools.partial(shards, mesh.shape["rows"], mesh.shape["tp"], mesh.shape["unit"]),
        mesh=mesh,
        in_specs=(
            P(("unit", "rows"), "tp"),
            P(("unit", "rows"), None),
            P("unit", "tp"),
            P(("unit", "rows"), "tp"),
            P(("unit", "rows"), None),
            P("unit", "tp"),
            P(("unit", "rows"), "tp"),
            P(("unit", "rows"), None),
            P("unit", "tp"),
            P(("unit", "tp"), "rows"),
            P(("unit", "tp"), None),
            P("unit", "rows"),
            P(("unit", "rows", "tp")),
            P(("unit", "rows", "tp")),
        ),
        out_specs=(
            P("unit", "tp"),
            P("unit", "tp"),
            P("unit", "tp"),
            P(("unit", "tp"), None),
            P("unit"),
        ),
        check_vma=False,
    )
```

```python
import functools

import jax
import jax.numpy as jnp
from jax import lax
from jax.experimental import pallas as pl
from jax.experimental.pallas import tpu as pltpu
from jax.sharding import PartitionSpec as P

MESH = pl.DeviceIdType.MESH
mix_rate = 0.5
order = (1, 0, 3, 2)
late_kind = order[-1]


def pieces_of(rows, firsts):
    sizes = [size for size in firsts if sum(firsts) < rows]
    left = rows - sum(sizes)
    return [*sizes, left] if left % 16 == 0 or not sizes else [rows]


def rounds_of(tps, t):
    if tps & (tps - 1):
        return [[(lax.rem(t + step, tps), t, lax.rem(t + tps - step, tps), 1) for step in range(1, tps)]]
    rounds, size = [], 1
    while size < tps:
        side = lax.rem(t // size, 2)
        base = (t // size) * size
        across = size - 2 * size * side
        rounds.append([(t + across, base, base + across, size)])
        size *= 2
    return rounds


def block_of(size, options):
    for option in options:
        if size % option == 0:
            return option
    return size


def kernel(n, tps, units, stacked, pieces, *refs):
    kinds = len(pieces)
    w, low, high = refs[:kinds], refs[kinds : 2 * kinds], refs[2 * kinds : 3 * kinds]
    norm_train, norm_step = refs[3 * kinds : 3 * kinds + 2]
    refs = refs[3 * kinds + 2 :]
    out, norm_out = refs[:kinds], refs[kinds]
    refs = refs[kinds + 1 :]
    w_own, low_own, high_own = refs[:kinds], refs[kinds : 2 * kinds], refs[2 * kinds : 3 * kinds]
    low_rows = refs[3 * kinds : 4 * kinds]
    refs = refs[4 * kinds :]
    norm_own, norm_all, norm_sem, load_sem, side_sem, send_sem, recv_sem, pass_send, pass_recv, norm_send, norm_recv, down_sem, cross_send, cross_recv = refs

    z, t = lax.axis_index("rows"), lax.axis_index("tp")
    late = lax.axis_index("unit") == units - 1
    rounds = rounds_of(tps, t)
    chunks = [(k, p) for k in order for p in range(len(pieces[k]))]
    has_up, has_down = z < n - 1, z > 0
    middle, top = n // 2, z == n - 1
    greeted = (has_up & (z >= middle), has_down & (z <= middle))
    waits = (has_up & ~greeted[0], has_down & ~greeted[1])
    held_up, held_down = late & (z == n - 2), late & (z == 1)
    missing_up, missing_down = late & (z == n - 1), late & (z == 0)

    def sends(k, direction):
        has, held = ((has_up, held_up), (has_down, held_down))[direction]
        return has & ~held if k == late_kind else has

    def comes(k, d, direction):
        has, missing = ((z - d >= 0, missing_up), (z + d < n, missing_down))[direction]
        return has & ~missing if k == late_kind else has

    def rows_of(k, p):
        return sum(pieces[k][:p]), pieces[k][p]

    def load(i):
        k, p = chunks[i]
        start, size = rows_of(k, p)
        return pltpu.make_async_copy(
            w[k].at[pl.ds(start, size)], w_own[k].at[pl.ds(start, size)], load_sem.at[i]
        )

    def side(k):
        return (
            pltpu.make_async_copy(low[k], low_own[k], side_sem.at[0, k]),
            pltpu.make_async_copy(high[k], high_own[k], side_sem.at[1, k]),
        )

    def load_kind(kind):
        for copy in side(kind):
            copy.start()
        for i, (k, p) in enumerate(chunks):
            if k == kind:
                load(i).start()

    barrier = pltpu.get_barrier_semaphore()

    @pl.when(z < middle)
    def _():
        pl.semaphore_signal(barrier, inc=1, device_id={"rows": z + 1}, device_id_type=MESH)

    @pl.when(z > middle)
    def _():
        pl.semaphore_signal(barrier, inc=1, device_id={"rows": z - 1}, device_id_type=MESH)

    @pl.when(top)
    def _():
        for partner in [exchange[0] for exchanges in rounds for exchange in exchanges]:
            pl.semaphore_signal(barrier, inc=1, device_id={"tp": partner}, device_id_type=MESH)

    for kind in order:
        load_kind(kind)

    norm_loads = [
        pltpu.make_async_copy(source, norm_own.at[j], norm_sem.at[j])
        for j, source in enumerate((norm_train, norm_step))
    ]
    for copy in norm_loads:
        copy.start()

    def region(k, p, origin):
        start, size = (0, w[k].shape[0]) if p is None else rows_of(k, p)
        columns = w[k].shape[1]
        if stacked[k]:
            return out[k].at[origin, pl.ds(start, size)]
        if out[k].shape[1] == columns:
            rows = w[k].shape[0]
            return out[k].at[pl.ds(pl.multiple_of(origin * rows + start, 16), size)]
        return out[k].at[pl.ds(start, size), pl.ds(pl.multiple_of(origin * columns, 128), columns)]

    def hop(place, send, recv, direction):
        return pltpu.make_async_remote_copy(
            src_ref=place,
            dst_ref=place,
            send_sem=send,
            recv_sem=recv,
            device_id={"rows": z + 1 - 2 * direction},
            device_id_type=MESH,
        )

    def chunk_hop(i, origin, direction):
        k, p = chunks[i]
        return hop(region(k, p, origin), send_sem.at[direction, i], recv_sem.at[direction, i], direction)

    def whole_hop(k, origin, direction):
        return hop(
            region(k, None, origin),
            pass_send.at[origin, k],
            pass_recv.at[origin, k],
            direction,
        )

    def norm_hop(origin):
        return pltpu.make_async_remote_copy(
            src_ref=norm_all.at[origin, t],
            dst_ref=norm_all.at[origin, t],
            send_sem=norm_send.at[origin],
            recv_sem=norm_recv.at[origin],
            device_id={"rows": z + 1},
            device_id_type=MESH,
        )

    def norm_down():
        return pltpu.make_async_remote_copy(
            src_ref=norm_out,
            dst_ref=norm_out,
            send_sem=down_sem.at[0],
            recv_sem=down_sem.at[1],
            device_id={"rows": z - 1},
            device_id_type=MESH,
        )

    def cross(r, j, coming=False):
        partner, base, theirs, size = rounds[r][j]
        place = norm_all.at[:, pl.ds(theirs if coming else base, size)]
        return pltpu.make_async_remote_copy(
            src_ref=place,
            dst_ref=place,
            send_sem=cross_send.at[r, j],
            recv_sem=cross_recv.at[r, j],
            device_id={"tp": partner},
            device_id_type=MESH,
        )

    def cross_start(r):
        for j in range(len(rounds[r])):
            cross(r, j).start()

    def cross_wait(r):
        for j in range(len(rounds[r])):
            cross(r, j, coming=True).wait_recv()

    def send_greeted(i):
        for direction in range(2):

            @pl.when(sends(chunks[i][0], direction) & greeted[direction])
            def _():
                chunk_hop(i, z, direction).start()

    def send_late():
        for direction in range(2):

            @pl.when(waits[direction])
            def _():
                chunk_hop(0, z + 1 - 2 * direction, 1 - direction).wait_recv()
                if direction == 0:
                    norm_hop(z).start()
                for i, (k, _) in enumerate(chunks):

                    @pl.when(sends(k, direction))
                    def _():
                        chunk_hop(i, z, direction).start()

    def merge(i):
        k, p = chunks[i]
        start, size = rows_of(k, p)
        columns = w[k].shape[1]
        high_block = block_of(size, (160, 128, 64, 32, 16))
        wide_block = block_of(columns, (256, 128))
        wides = columns // wide_block
        place = region(k, p, z)

        def body(b, _):
            if size == high_block:
                r, c = 0, b
            else:
                r, c = b // wides, b % wides
            r = r * high_block
            c = 0 if wides == 1 else pl.multiple_of(c * wide_block, wide_block)
            mine = pl.ds(start + r, high_block)
            wide = pl.ds(c, wide_block)
            result = w_own[k][mine, wide].astype(jnp.float32) + mix_rate * jnp.dot(
                low_rows[k][mine, :], high_own[k][:, wide], preferred_element_type=jnp.float32
            )
            place[pl.ds(r, high_block), wide] = result.astype(jnp.bfloat16)
            return 0

        lax.fori_loop(0, (size // high_block) * wides, body, 0)

    for i, (k, p) in enumerate(chunks):
        if p == 0:
            for copy in side(k):
                copy.wait()
        mine = pl.ds(*rows_of(k, p))
        low_rows[k][mine, :] = low_own[k][:, mine].astype(jnp.float32).T.astype(jnp.bfloat16)
        if i == 1:
            partners = greeted[0].astype(jnp.int32) + greeted[1].astype(jnp.int32)
            partners += top.astype(jnp.int32) * sum(map(len, rounds))

            @pl.when(partners > 0)
            def _():
                pl.semaphore_wait(barrier, partners)

        if i > 0:
            send_greeted(i - 1)
        load(i).wait()
        merge(i)
        if i == min(3, len(chunks) - 2):
            for copy in norm_loads:
                copy.wait()
            norm_all[z, t] = (norm_own[0] + norm_own[1]).astype(jnp.bfloat16).astype(jnp.float32)
        if i == min(4, len(chunks) - 1):

            @pl.when(greeted[0])
            def _():
                norm_hop(z).start()

    send_greeted(len(chunks) - 1)
    send_late()

    def arrival(arrived, onward, d, k, near):
        for direction, origin in ((0, z - d), (1, z + d)):

            @pl.when(comes(k, d, direction))
            def _():
                for j, make in enumerate(arrived):
                    if near and k == order[0] and j == 0:

                        @pl.when(~waits[1 - direction])
                        def _():
                            make(origin, direction).wait_recv()

                    else:
                        make(origin, direction).wait_recv()

                @pl.when(sends(k, direction))
                def _():
                    onward(origin, direction).start()

    def distance(d, _, near=False):
        @pl.when(z - d >= 0)
        def _():
            norm_hop(z - d).wait_recv()

            @pl.when(has_up)
            def _():
                norm_hop(z - d).start()

        for j, k in enumerate(order):

            @pl.when(top & (d == n - 1))
            def _():
                if j == 0:
                    share_norm()
                if j == 1:
                    norm_down().start()

            onward = functools.partial(whole_hop, k)
            arrived = [onward]
            if near:
                arrived = [functools.partial(chunk_hop, i) for i, c in enumerate(chunks) if c[0] == k]
            arrival(arrived, onward, d, k, near)
        return 0

    def share_norm():
        for r in range(len(rounds)):
            cross_start(r)
            cross_wait(r)
        write_norm()

    def write_norm():
        line = jnp.concatenate([norm_all[a, b] for a in range(n) for b in range(tps)], axis=1)
        width = norm_out.shape[1]
        norm_out[...] = jnp.concatenate(
            [line[:, a * width : (a + 1) * width] for a in range(norm_out.shape[0])], axis=0
        ).astype(jnp.bfloat16)

    distance(jnp.int32(1), 0, near=True)
    lax.fori_loop(2, n, distance, 0)

    @pl.when(has_up)
    def _():
        norm_down().wait_recv()

    @pl.when(has_up & has_down)
    def _():
        norm_down().start()

    for direction in range(2):
        for i in range(len(chunks)):

            @pl.when(sends(chunks[i][0], direction))
            def _():
                chunk_hop(i, z, direction).wait_send()

    @pl.when(has_up)
    def _():
        norm_hop(z).wait_send()

    @pl.when(has_down)
    def _():
        norm_down().wait_send()

    def drain(origin, _):
        for direction, passed in ((0, origin < z), (1, origin > z)):
            for k in range(kinds):

                @pl.when(sends(k, direction) & passed)
                def _():
                    whole_hop(k, origin, direction).wait_send()

        @pl.when(has_up & (origin < z))
        def _():
            norm_hop(origin).wait_send()

        return 0

    lax.fori_loop(0, n, drain, 0)

    @pl.when(top)
    def _():
        for r in range(len(rounds)):
            for j in range(len(rounds[r])):
                cross(r, j).wait_send()


def ends(n, units):
    z, late = lax.axis_index("rows"), lax.axis_index("unit") == units - 1
    return late & (z == 0), late & (z == n - 1)


def put(n, units, parts, *refs):
    kinds = len(parts)
    src, dst, sem = refs[:kinds], refs[kinds : 2 * kinds], refs[-1]
    bottom, top = ends(n, units)
    copies, kept = [], []
    for k in range(kinds):
        size = src[k].shape[0] // parts[k]
        for p in range(parts[k]):
            rows = pl.ds(p * size, size)
            copy = pltpu.make_async_copy(src[k].at[rows], dst[k].at[rows], sem.at[len(copies) + len(kept)])
            (kept if k == late_kind else copies).append(copy)
    share = src[late_kind].shape[0] // n

    def own(origin):
        rows = pl.ds(origin * share, share)
        return pltpu.make_async_copy(src[late_kind].at[rows], dst[late_kind].at[rows], sem.at[sum(parts)])

    for copy in copies:
        copy.start()

    @pl.when(~bottom & ~top)
    def _():
        for copy in kept:
            copy.start()
        for copy in kept:
            copy.wait()

    for flag, origin in ((bottom, 0), (top, n - 1)):

        @pl.when(flag)
        def _():
            own(origin).start()
            own(origin).wait()

    for copy in copies:
        copy.wait()


def place(n, units, arrays):
    parts = [2 if x.shape[0] % 128 == 0 else 1 for x in arrays]
    vmem, hbm = pl.BlockSpec(memory_space=pltpu.VMEM), pl.BlockSpec(memory_space=pltpu.HBM)
    return pl.pallas_call(
        functools.partial(put, n, units, parts),
        out_shape=[pltpu.HBM(x.shape, x.dtype) for x in arrays] + [pltpu.VMEM((8, 128), jnp.float32)],
        in_specs=[vmem] * len(arrays),
        out_specs=[hbm] * len(arrays) + [vmem],
        scratch_shapes=[pltpu.SemaphoreType.DMA((sum(parts) + 1,))],
        compiler_params=pltpu.CompilerParams(vmem_limit_bytes=24 * 1024 * 1024),
        name="place",
    )(*arrays)


def last_hop(n, units, have, after, got, send_sem, recv_sem):
    z, late = lax.axis_index("rows"), lax.axis_index("unit") == units - 1
    bottom, top = ends(n, units)
    size = got.shape[0]
    share = have.shape[0] - size

    def hop(direction):
        return pltpu.make_async_remote_copy(
            src_ref=have.at[pl.ds(share * direction, size)],
            dst_ref=got,
            send_sem=send_sem.at[direction],
            recv_sem=recv_sem.at[direction],
            device_id={"rows": z + 1 - 2 * direction},
            device_id_type=MESH,
        )

    barrier = pltpu.get_barrier_semaphore()
    above, below = late & (z == n - 2), late & (z == 1)

    @pl.when(bottom)
    def _():
        pl.semaphore_signal(barrier, inc=1, device_id={"rows": z + 1}, device_id_type=MESH)

    @pl.when(top)
    def _():
        pl.semaphore_signal(barrier, inc=1, device_id={"rows": z - 1}, device_id_type=MESH)

    @pl.when(above | below)
    def _():
        pl.semaphore_wait(barrier, above.astype(jnp.int32) + below.astype(jnp.int32))

    for direction, flag in ((0, above), (1, below)):

        @pl.when(flag)
        def _():
            hop(direction).start()

    for direction, flag in ((0, top), (1, bottom)):

        @pl.when(flag)
        def _():
            hop(direction).wait_recv()

    for direction, flag in ((0, above), (1, below)):

        @pl.when(flag)
        def _():
            hop(direction).wait_send()


def finish(n, units, have, after):
    share = have.shape[0] // n
    vmem, dma = pl.BlockSpec(memory_space=pltpu.VMEM), pltpu.SemaphoreType.DMA
    return pl.pallas_call(
        functools.partial(last_hop, n, units),
        out_shape=pltpu.VMEM((have.shape[0] - share, have.shape[1]), have.dtype),
        in_specs=[vmem, vmem],
        out_specs=vmem,
        scratch_shapes=[dma((2,)), dma((2,))],
        compiler_params=pltpu.CompilerParams(
            collective_id=1, has_side_effects=True, vmem_limit_bytes=4 * 1024 * 1024
        ),
        name="last_hop",
    )(have, after)


def add_rows(n, units, got, old, out, sem):
    size = got.shape[0]
    share = out.shape[0] - size
    for flag, start in zip(ends(n, units), (share, 0)):

        @pl.when(flag)
        def _():
            copy = pltpu.make_async_copy(got, out.at[pl.ds(start, size)], sem)
            copy.start()
            copy.wait()


def complete(n, units, got, old):
    vmem, hbm = pl.BlockSpec(memory_space=pltpu.VMEM), pl.BlockSpec(memory_space=pltpu.HBM)
    return pl.pallas_call(
        functools.partial(add_rows, n, units),
        out_shape=pltpu.HBM(old.shape, old.dtype),
        in_specs=[vmem, hbm],
        out_specs=hbm,
        scratch_shapes=[pltpu.SemaphoreType.DMA],
        input_output_aliases={1: 0},
        compiler_params=pltpu.CompilerParams(vmem_limit_bytes=4 * 1024 * 1024),
        name="complete",
    )(got, old)


def shards(n, tps, units, *args):
    w, low, high = args[0:12:3], [x.T for x in args[1:12:3]], args[2:12:3]
    norm_train, norm_step = args[12].reshape(1, -1), args[13].reshape(1, -1)
    kinds = len(w)
    by_column = [False] * (kinds - 1) + [True]
    stacked = [by_column[k] and w[k].shape[1] % 128 != 0 for k in range(kinds)]
    firsts = {order[0]: (128, 128), order[1]: ()}
    pieces = [pieces_of(w[k].shape[0], firsts.get(k, ())) for k in range(kinds)]
    count = sum(map(len, pieces))
    rounds = rounds_of(tps, 0)
    crossings = (len(rounds), max(map(len, rounds), default=0))
    shapes = []
    for k in range(kinds):
        rows, columns = w[k].shape
        if stacked[k]:
            shapes.append((n, rows, columns))
        elif by_column[k]:
            shapes.append((rows, n * columns))
        else:
            shapes.append((n * rows, columns))
    share = norm_train.shape[1]
    total = n * tps * share
    width = 128 if total % 128 == 0 else total
    vmem, hbm = pl.BlockSpec(memory_space=pltpu.VMEM), pl.BlockSpec(memory_space=pltpu.HBM)
    dma = pltpu.SemaphoreType.DMA
    operands = (*w, *low, *high, norm_train, norm_step)
    results = pl.pallas_call(
        functools.partial(kernel, n, tps, units, stacked, pieces),
        out_shape=[pltpu.VMEM(s, jnp.bfloat16) for s in shapes]
        + [pltpu.VMEM((total // width, width), jnp.bfloat16)],
        in_specs=[hbm] * (3 * kinds + 2),
        out_specs=[vmem] * (kinds + 1),
        scratch_shapes=[pltpu.VMEM(x.shape, x.dtype) for x in (*w, *low, *high)]
        + [pltpu.VMEM(x.shape[::-1], x.dtype) for x in low]
        + [
            pltpu.VMEM((2, 1, share), jnp.float32),
            pltpu.VMEM((n, tps, 1, share), jnp.float32),
            dma((2,)),
            dma((count,)),
            dma((2, kinds)),
            dma((2, count)),
            dma((2, count)),
            dma((n, kinds)),
            dma((n, kinds)),
            dma((n,)),
            dma((n,)),
            dma((2,)),
            dma(crossings),
            dma(crossings),
        ],
        compiler_params=pltpu.CompilerParams(
            collective_id=0, has_side_effects=True, vmem_limit_bytes=24 * 1024 * 1024
        ),
        name="merge_and_gather",
    )(*[pltpu.with_memory_space_constraint(x, pltpu.HBM) for x in operands])
    have = results[late_kind]
    *results, after = place(n, units, results)
    if n > 1:
        results[late_kind] = complete(n, units, finish(n, units, have, after), results[late_kind])
    finals = []
    for k in range(kinds):
        full = results[k]
        if stacked[k]:
            full = full.transpose(1, 0, 2).reshape(full.shape[1], -1)
        finals.append(full)
    return (*finals, results[kinds].reshape(-1))


def solution(mesh):
    return jax.shard_map(
        functools.partial(shards, mesh.shape["rows"], mesh.shape["tp"], mesh.shape["unit"]),
        mesh=mesh,
        in_specs=(
            P(("unit", "rows"), "tp"),
            P(("unit", "rows"), None),
            P("unit", "tp"),
            P(("unit", "rows"), "tp"),
            P(("unit", "rows"), None),
            P("unit", "tp"),
            P(("unit", "rows"), "tp"),
            P(("unit", "rows"), None),
            P("unit", "tp"),
            P(("unit", "tp"), "rows"),
            P(("unit", "tp"), None),
            P("unit", "rows"),
            P(("unit", "rows", "tp")),
            P(("unit", "rows", "tp")),
        ),
        out_specs=(
            P("unit", "tp"),
            P("unit", "tp"),
            P("unit", "tp"),
            P(("unit", "tp"), None),
            P("unit"),
        ),
        check_vma=False,
    )
```

```python
import functools

import jax
import jax.numpy as jnp
from jax import lax
from jax.experimental import pallas as pl
from jax.experimental.pallas import tpu as pltpu
from jax.sharding import PartitionSpec as P

MESH = pl.DeviceIdType.MESH
mix_rate = 0.5
order = (1, 0, 3, 2)
late_kind = order[-1]


def pieces_of(rows, firsts):
    sizes = [size for size in firsts if sum(firsts) < rows]
    left = rows - sum(sizes)
    return [*sizes, left] if left % 16 == 0 or not sizes else [rows]


def rounds_of(tps, t):
    if tps & (tps - 1):
        return [[(lax.rem(t + step, tps), t, lax.rem(t + tps - step, tps), 1) for step in range(1, tps)]]
    rounds, size = [], 1
    while size < tps:
        side = lax.rem(t // size, 2)
        base = (t // size) * size
        across = size - 2 * size * side
        rounds.append([(t + across, base, base + across, size)])
        size *= 2
    return rounds


def block_of(size, options):
    for option in options:
        if size % option == 0:
            return option
    return size


def kernel(n, tps, units, stacked, pieces, *refs):
    kinds = len(pieces)
    w, low, high = refs[:kinds], refs[kinds : 2 * kinds], refs[2 * kinds : 3 * kinds]
    norm_train, norm_step = refs[3 * kinds : 3 * kinds + 2]
    refs = refs[3 * kinds + 2 :]
    out, norm_out = refs[:kinds], refs[kinds]
    refs = refs[kinds + 1 :]
    w_own, low_own, high_own = refs[:kinds], refs[kinds : 2 * kinds], refs[2 * kinds : 3 * kinds]
    low_rows = refs[3 * kinds : 4 * kinds]
    refs = refs[4 * kinds :]
    norm_own, norm_all, norm_sem, load_sem, side_sem, send_sem, recv_sem, pass_send, pass_recv, norm_send, norm_recv, down_sem, cross_send, cross_recv = refs

    z, t = lax.axis_index("rows"), lax.axis_index("tp")
    late = lax.axis_index("unit") == units - 1
    rounds = rounds_of(tps, t)
    chunks = [(k, p) for k in order for p in range(len(pieces[k]))]
    has_up, has_down = z < n - 1, z > 0
    middle, top = n // 2, z == n - 1
    greeted = (has_up & (z >= middle), has_down & (z <= middle))
    waits = (has_up & ~greeted[0], has_down & ~greeted[1])
    held_up, held_down = late & (z == n - 2), late & (z == 1)
    missing_up, missing_down = late & (z == n - 1), late & (z == 0)

    def sends(k, direction):
        has, held = ((has_up, held_up), (has_down, held_down))[direction]
        return has & ~held if k == late_kind else has

    def comes(k, d, direction):
        has, missing = ((z - d >= 0, missing_up), (z + d < n, missing_down))[direction]
        return has & ~missing if k == late_kind else has

    def rows_of(k, p):
        return sum(pieces[k][:p]), pieces[k][p]

    def load(i):
        k, p = chunks[i]
        start, size = rows_of(k, p)
        return pltpu.make_async_copy(
            w[k].at[pl.ds(start, size)], w_own[k].at[pl.ds(start, size)], load_sem.at[i]
        )

    def side(k):
        return (
            pltpu.make_async_copy(low[k], low_own[k], side_sem.at[0, k]),
            pltpu.make_async_copy(high[k], high_own[k], side_sem.at[1, k]),
        )

    def load_kind(kind):
        for copy in side(kind):
            copy.start()
        for i, (k, p) in enumerate(chunks):
            if k == kind:
                load(i).start()

    barrier = pltpu.get_barrier_semaphore()

    @pl.when(z < middle)
    def _():
        pl.semaphore_signal(barrier, inc=1, device_id={"rows": z + 1}, device_id_type=MESH)

    @pl.when(z > middle)
    def _():
        pl.semaphore_signal(barrier, inc=1, device_id={"rows": z - 1}, device_id_type=MESH)

    @pl.when(top)
    def _():
        for partner in [exchange[0] for exchanges in rounds for exchange in exchanges]:
            pl.semaphore_signal(barrier, inc=1, device_id={"tp": partner}, device_id_type=MESH)

    for kind in order:
        load_kind(kind)

    norm_loads = [
        pltpu.make_async_copy(source, norm_own.at[j], norm_sem.at[j])
        for j, source in enumerate((norm_train, norm_step))
    ]
    for copy in norm_loads:
        copy.start()

    def region(k, p, origin):
        start, size = (0, w[k].shape[0]) if p is None else rows_of(k, p)
        columns = w[k].shape[1]
        if stacked[k]:
            return out[k].at[origin, pl.ds(start, size)]
        if out[k].shape[1] == columns:
            rows = w[k].shape[0]
            return out[k].at[pl.ds(pl.multiple_of(origin * rows + start, 16), size)]
        return out[k].at[pl.ds(start, size), pl.ds(pl.multiple_of(origin * columns, 128), columns)]

    def hop(place, send, recv, direction):
        return pltpu.make_async_remote_copy(
            src_ref=place,
            dst_ref=place,
            send_sem=send,
            recv_sem=recv,
            device_id={"rows": z + 1 - 2 * direction},
            device_id_type=MESH,
        )

    def chunk_hop(i, origin, direction):
        k, p = chunks[i]
        return hop(region(k, p, origin), send_sem.at[direction, i], recv_sem.at[direction, i], direction)

    def whole_hop(k, origin, direction):
        return hop(
            region(k, None, origin),
            pass_send.at[origin, k],
            pass_recv.at[origin, k],
            direction,
        )

    def norm_hop(origin):
        return pltpu.make_async_remote_copy(
            src_ref=norm_all.at[origin, t],
            dst_ref=norm_all.at[origin, t],
            send_sem=norm_send.at[origin],
            recv_sem=norm_recv.at[origin],
            device_id={"rows": z + 1},
            device_id_type=MESH,
        )

    def norm_down():
        return pltpu.make_async_remote_copy(
            src_ref=norm_out,
            dst_ref=norm_out,
            send_sem=down_sem.at[0],
            recv_sem=down_sem.at[1],
            device_id={"rows": z - 1},
            device_id_type=MESH,
        )

    def cross(r, j, coming=False):
        partner, base, theirs, size = rounds[r][j]
        place = norm_all.at[:, pl.ds(theirs if coming else base, size)]
        return pltpu.make_async_remote_copy(
            src_ref=place,
            dst_ref=place,
            send_sem=cross_send.at[r, j],
            recv_sem=cross_recv.at[r, j],
            device_id={"tp": partner},
            device_id_type=MESH,
        )

    def cross_start(r):
        for j in range(len(rounds[r])):
            cross(r, j).start()

    def cross_wait(r):
        for j in range(len(rounds[r])):
            cross(r, j, coming=True).wait_recv()

    def send_greeted(i):
        for direction in range(2):

            @pl.when(sends(chunks[i][0], direction) & greeted[direction])
            def _():
                chunk_hop(i, z, direction).start()

    def send_late():
        for direction in range(2):

            @pl.when(waits[direction])
            def _():
                chunk_hop(0, z + 1 - 2 * direction, 1 - direction).wait_recv()
                if direction == 0:
                    norm_hop(z).start()
                for i, (k, _) in enumerate(chunks):

                    @pl.when(sends(k, direction))
                    def _():
                        chunk_hop(i, z, direction).start()

    def merge(i):
        k, p = chunks[i]
        start, size = rows_of(k, p)
        columns = w[k].shape[1]
        high_block = block_of(size, (160, 128, 64, 32, 16))
        wide_block = block_of(columns, (256, 128))
        wides = columns // wide_block
        place = region(k, p, z)

        def body(b, _):
            if size == high_block:
                r, c = 0, b
            else:
                r, c = b // wides, b % wides
            r = r * high_block
            c = 0 if wides == 1 else pl.multiple_of(c * wide_block, wide_block)
            mine = pl.ds(start + r, high_block)
            wide = pl.ds(c, wide_block)
            result = w_own[k][mine, wide].astype(jnp.float32) + mix_rate * jnp.dot(
                low_rows[k][mine, :], high_own[k][:, wide], preferred_element_type=jnp.float32
            )
            place[pl.ds(r, high_block), wide] = result.astype(jnp.bfloat16)
            return 0

        lax.fori_loop(0, (size // high_block) * wides, body, 0)

    for i, (k, p) in enumerate(chunks):
        if p == 0:
            for copy in side(k):
                copy.wait()
        mine = pl.ds(*rows_of(k, p))
        low_rows[k][mine, :] = low_own[k][:, mine].astype(jnp.float32).T.astype(jnp.bfloat16)
        if i == 1:
            partners = greeted[0].astype(jnp.int32) + greeted[1].astype(jnp.int32)
            partners += top.astype(jnp.int32) * sum(map(len, rounds))

            @pl.when(partners > 0)
            def _():
                pl.semaphore_wait(barrier, partners)

        if i > 0:
            send_greeted(i - 1)
        load(i).wait()
        merge(i)
        if i == min(3, len(chunks) - 2):
            for copy in norm_loads:
                copy.wait()
            norm_all[z, t] = (norm_own[0] + norm_own[1]).astype(jnp.bfloat16).astype(jnp.float32)
        if i == min(4, len(chunks) - 1):

            @pl.when(greeted[0])
            def _():
                norm_hop(z).start()

    send_greeted(len(chunks) - 1)
    send_late()

    def arrival(arrived, onward, d, k, near):
        for direction, origin in ((0, z - d), (1, z + d)):

            @pl.when(comes(k, d, direction))
            def _():
                for j, make in enumerate(arrived):
                    if near and k == order[0] and j == 0:

                        @pl.when(~waits[1 - direction])
                        def _():
                            make(origin, direction).wait_recv()

                    else:
                        make(origin, direction).wait_recv()

                @pl.when(sends(k, direction))
                def _():
                    onward(origin, direction).start()

    def distance(d, _, near=False):
        @pl.when(z - d >= 0)
        def _():
            norm_hop(z - d).wait_recv()

            @pl.when(has_up)
            def _():
                norm_hop(z - d).start()

        for j, k in enumerate(order):

            @pl.when(top & (d == n - 1))
            def _():
                if j == 0:
                    share_norm()
                if j == 1:
                    norm_down().start()

            onward = functools.partial(whole_hop, k)
            arrived = [onward]
            if near:
                arrived = [functools.partial(chunk_hop, i) for i, c in enumerate(chunks) if c[0] == k]
            arrival(arrived, onward, d, k, near)
        return 0

    def share_norm():
        for r in range(len(rounds)):
            cross_start(r)
            cross_wait(r)
        write_norm()

    def write_norm():
        line = jnp.concatenate([norm_all[a, b] for a in range(n) for b in range(tps)], axis=1)
        width = norm_out.shape[1]
        norm_out[...] = jnp.concatenate(
            [line[:, a * width : (a + 1) * width] for a in range(norm_out.shape[0])], axis=0
        ).astype(jnp.bfloat16)

    distance(jnp.int32(1), 0, near=True)
    lax.fori_loop(2, n, distance, 0)

    @pl.when(has_up)
    def _():
        norm_down().wait_recv()

    @pl.when(has_up & has_down)
    def _():
        norm_down().start()

    for direction in range(2):
        for i in range(len(chunks)):

            @pl.when(sends(chunks[i][0], direction))
            def _():
                chunk_hop(i, z, direction).wait_send()

    @pl.when(has_up)
    def _():
        norm_hop(z).wait_send()

    @pl.when(has_down)
    def _():
        norm_down().wait_send()

    def drain(origin, _):
        for direction, passed in ((0, origin < z), (1, origin > z)):
            for k in range(kinds):

                @pl.when(sends(k, direction) & passed)
                def _():
                    whole_hop(k, origin, direction).wait_send()

        @pl.when(has_up & (origin < z))
        def _():
            norm_hop(origin).wait_send()

        return 0

    lax.fori_loop(0, n, drain, 0)

    @pl.when(top)
    def _():
        for r in range(len(rounds)):
            for j in range(len(rounds[r])):
                cross(r, j).wait_send()


def ends(n, units):
    z, late = lax.axis_index("rows"), lax.axis_index("unit") == units - 1
    return late & (z == 0), late & (z == n - 1)


def put(n, units, parts, *refs):
    kinds = len(parts)
    src, dst, sem = refs[:kinds], refs[kinds : 2 * kinds], refs[-1]
    bottom, top = ends(n, units)
    copies, kept = [], []
    for k in range(kinds):
        size = src[k].shape[0] // parts[k]
        for p in range(parts[k]):
            rows = pl.ds(p * size, size)
            copy = pltpu.make_async_copy(src[k].at[rows], dst[k].at[rows], sem.at[len(copies) + len(kept)])
            (kept if k == late_kind else copies).append(copy)
    share = src[late_kind].shape[0] // n

    def own(origin):
        rows = pl.ds(origin * share, share)
        return pltpu.make_async_copy(src[late_kind].at[rows], dst[late_kind].at[rows], sem.at[sum(parts)])

    for copy in copies:
        copy.start()

    @pl.when(~bottom & ~top)
    def _():
        for copy in kept:
            copy.start()
        for copy in kept:
            copy.wait()

    for flag, origin in ((bottom, 0), (top, n - 1)):

        @pl.when(flag)
        def _():
            own(origin).start()
            own(origin).wait()

    for copy in copies:
        copy.wait()


def place(n, units, arrays):
    parts = [2 if x.shape[0] % 128 == 0 else 1 for x in arrays]
    vmem, hbm = pl.BlockSpec(memory_space=pltpu.VMEM), pl.BlockSpec(memory_space=pltpu.HBM)
    return pl.pallas_call(
        functools.partial(put, n, units, parts),
        out_shape=[pltpu.HBM(x.shape, x.dtype) for x in arrays] + [pltpu.VMEM((8, 128), jnp.float32)],
        in_specs=[vmem] * len(arrays),
        out_specs=[hbm] * len(arrays) + [vmem],
        scratch_shapes=[pltpu.SemaphoreType.DMA((sum(parts) + 1,))],
        compiler_params=pltpu.CompilerParams(vmem_limit_bytes=24 * 1024 * 1024),
        name="place",
    )(*arrays)


def last_hop(n, units, have, after, got, send_sem, recv_sem):
    z, late = lax.axis_index("rows"), lax.axis_index("unit") == units - 1
    bottom, top = ends(n, units)
    size = got.shape[0]
    share = have.shape[0] - size

    def hops(direction):
        return [
            pltpu.make_async_remote_copy(
                src_ref=have.at[pl.ds(share * (direction + j), share)],
                dst_ref=got.at[pl.ds(share * j, share)],
                send_sem=send_sem.at[direction, j],
                recv_sem=recv_sem.at[direction, j],
                device_id={"rows": z + 1 - 2 * direction},
                device_id_type=MESH,
            )
            for j in range(n - 1)
        ]

    barrier = pltpu.get_barrier_semaphore()
    above, below = late & (z == n - 2), late & (z == 1)

    @pl.when(bottom)
    def _():
        pl.semaphore_signal(barrier, inc=1, device_id={"rows": z + 1}, device_id_type=MESH)

    @pl.when(top)
    def _():
        pl.semaphore_signal(barrier, inc=1, device_id={"rows": z - 1}, device_id_type=MESH)

    @pl.when(above | below)
    def _():
        pl.semaphore_wait(barrier, above.astype(jnp.int32) + below.astype(jnp.int32))

    for direction, flag in ((0, above), (1, below)):

        @pl.when(flag)
        def _():
            for hop in hops(direction):
                hop.start()

    for direction, flag in ((0, top), (1, bottom)):

        @pl.when(flag)
        def _():
            for hop in hops(direction):
                hop.wait_recv()

    for direction, flag in ((0, above), (1, below)):

        @pl.when(flag)
        def _():
            for hop in hops(direction):
                hop.wait_send()


def finish(n, units, have, after):
    share = have.shape[0] // n
    vmem, dma = pl.BlockSpec(memory_space=pltpu.VMEM), pltpu.SemaphoreType.DMA
    return pl.pallas_call(
        functools.partial(last_hop, n, units),
        out_shape=pltpu.VMEM((have.shape[0] - share, have.shape[1]), have.dtype),
        in_specs=[vmem, vmem],
        out_specs=vmem,
        scratch_shapes=[dma((2, n - 1)), dma((2, n - 1))],
        compiler_params=pltpu.CompilerParams(
            collective_id=1, has_side_effects=True, vmem_limit_bytes=4 * 1024 * 1024
        ),
        name="last_hop",
    )(have, after)


def add_rows(n, units, got, old, out, sem):
    size = got.shape[0]
    share = out.shape[0] - size
    for flag, start in zip(ends(n, units), (share, 0)):

        @pl.when(flag)
        def _():
            copy = pltpu.make_async_copy(got, out.at[pl.ds(start, size)], sem)
            copy.start()
            copy.wait()


def complete(n, units, got, old):
    vmem, hbm = pl.BlockSpec(memory_space=pltpu.VMEM), pl.BlockSpec(memory_space=pltpu.HBM)
    return pl.pallas_call(
        functools.partial(add_rows, n, units),
        out_shape=pltpu.HBM(old.shape, old.dtype),
        in_specs=[vmem, hbm],
        out_specs=hbm,
        scratch_shapes=[pltpu.SemaphoreType.DMA],
        input_output_aliases={1: 0},
        compiler_params=pltpu.CompilerParams(vmem_limit_bytes=4 * 1024 * 1024),
        name="complete",
    )(got, old)


def shards(n, tps, units, *args):
    w, low, high = args[0:12:3], [x.T for x in args[1:12:3]], args[2:12:3]
    norm_train, norm_step = args[12].reshape(1, -1), args[13].reshape(1, -1)
    kinds = len(w)
    by_column = [False] * (kinds - 1) + [True]
    stacked = [by_column[k] and w[k].shape[1] % 128 != 0 for k in range(kinds)]
    firsts = {order[0]: (128, 128), order[1]: ()}
    pieces = [pieces_of(w[k].shape[0], firsts.get(k, ())) for k in range(kinds)]
    count = sum(map(len, pieces))
    rounds = rounds_of(tps, 0)
    crossings = (len(rounds), max(map(len, rounds), default=0))
    shapes = []
    for k in range(kinds):
        rows, columns = w[k].shape
        if stacked[k]:
            shapes.append((n, rows, columns))
        elif by_column[k]:
            shapes.append((rows, n * columns))
        else:
            shapes.append((n * rows, columns))
    share = norm_train.shape[1]
    total = n * tps * share
    width = 128 if total % 128 == 0 else total
    vmem, hbm = pl.BlockSpec(memory_space=pltpu.VMEM), pl.BlockSpec(memory_space=pltpu.HBM)
    dma = pltpu.SemaphoreType.DMA
    operands = (*w, *low, *high, norm_train, norm_step)
    results = pl.pallas_call(
        functools.partial(kernel, n, tps, units, stacked, pieces),
        out_shape=[pltpu.VMEM(s, jnp.bfloat16) for s in shapes]
        + [pltpu.VMEM((total // width, width), jnp.bfloat16)],
        in_specs=[hbm] * (3 * kinds + 2),
        out_specs=[vmem] * (kinds + 1),
        scratch_shapes=[pltpu.VMEM(x.shape, x.dtype) for x in (*w, *low, *high)]
        + [pltpu.VMEM(x.shape[::-1], x.dtype) for x in low]
        + [
            pltpu.VMEM((2, 1, share), jnp.float32),
            pltpu.VMEM((n, tps, 1, share), jnp.float32),
            dma((2,)),
            dma((count,)),
            dma((2, kinds)),
            dma((2, count)),
            dma((2, count)),
            dma((n, kinds)),
            dma((n, kinds)),
            dma((n,)),
            dma((n,)),
            dma((2,)),
            dma(crossings),
            dma(crossings),
        ],
        compiler_params=pltpu.CompilerParams(
            collective_id=0, has_side_effects=True, vmem_limit_bytes=24 * 1024 * 1024
        ),
        name="merge_and_gather",
    )(*[pltpu.with_memory_space_constraint(x, pltpu.HBM) for x in operands])
    have = results[late_kind]
    *results, after = place(n, units, results)
    if n > 1:
        results[late_kind] = complete(n, units, finish(n, units, have, after), results[late_kind])
    finals = []
    for k in range(kinds):
        full = results[k]
        if stacked[k]:
            full = full.transpose(1, 0, 2).reshape(full.shape[1], -1)
        finals.append(full)
    return (*finals, results[kinds].reshape(-1))


def solution(mesh):
    return jax.shard_map(
        functools.partial(shards, mesh.shape["rows"], mesh.shape["tp"], mesh.shape["unit"]),
        mesh=mesh,
        in_specs=(
            P(("unit", "rows"), "tp"),
            P(("unit", "rows"), None),
            P("unit", "tp"),
            P(("unit", "rows"), "tp"),
            P(("unit", "rows"), None),
            P("unit", "tp"),
            P(("unit", "rows"), "tp"),
            P(("unit", "rows"), None),
            P("unit", "tp"),
            P(("unit", "tp"), "rows"),
            P(("unit", "tp"), None),
            P("unit", "rows"),
            P(("unit", "rows", "tp")),
            P(("unit", "rows", "tp")),
        ),
        out_specs=(
            P("unit", "tp"),
            P("unit", "tp"),
            P("unit", "tp"),
            P(("unit", "tp"), None),
            P("unit"),
        ),
        check_vma=False,
    )
```

```python
import functools

import jax
import jax.numpy as jnp
from jax import lax
from jax.experimental import pallas as pl
from jax.experimental.pallas import tpu as pltpu
from jax.sharding import PartitionSpec as P

MESH = pl.DeviceIdType.MESH
mix_rate = 0.5
order = (1, 0, 3, 2)
late_kind = order[-1]


def pieces_of(rows, firsts):
    sizes = [size for size in firsts if sum(firsts) < rows]
    left = rows - sum(sizes)
    return [*sizes, left] if left % 16 == 0 or not sizes else [rows]


def rounds_of(tps, t):
    if tps & (tps - 1):
        return [[(lax.rem(t + step, tps), t, lax.rem(t + tps - step, tps), 1) for step in range(1, tps)]]
    rounds, size = [], 1
    while size < tps:
        side = lax.rem(t // size, 2)
        base = (t // size) * size
        across = size - 2 * size * side
        rounds.append([(t + across, base, base + across, size)])
        size *= 2
    return rounds


def block_of(size, options):
    for option in options:
        if size % option == 0:
            return option
    return size


def kernel(n, tps, units, stacked, pieces, *refs):
    kinds = len(pieces)
    w, low, high = refs[:kinds], refs[kinds : 2 * kinds], refs[2 * kinds : 3 * kinds]
    norm_train, norm_step = refs[3 * kinds : 3 * kinds + 2]
    refs = refs[3 * kinds + 2 :]
    out, norm_out = refs[:kinds], refs[kinds]
    refs = refs[kinds + 1 :]
    w_own, low_own, high_own = refs[:kinds], refs[kinds : 2 * kinds], refs[2 * kinds : 3 * kinds]
    low_rows = refs[3 * kinds : 4 * kinds]
    refs = refs[4 * kinds :]
    norm_own, norm_all, norm_sem, load_sem, side_sem, send_sem, recv_sem, pass_send, pass_recv, norm_send, norm_recv, down_sem, cross_send, cross_recv = refs

    z, t = lax.axis_index("rows"), lax.axis_index("tp")
    late = lax.axis_index("unit") == units - 1
    rounds = rounds_of(tps, t)
    chunks = [(k, p) for k in order for p in range(len(pieces[k]))]
    has_up, has_down = z < n - 1, z > 0
    middle, top = n // 2, z == n - 1
    greeted = (has_up & (z >= middle), has_down & (z <= middle))
    waits = (has_up & ~greeted[0], has_down & ~greeted[1])
    held_up, held_down = late & (z == n - 2), late & (z == 1)
    missing_up, missing_down = late & (z == n - 1), late & (z == 0)

    def sends(k, direction):
        has, held = ((has_up, held_up), (has_down, held_down))[direction]
        return has & ~held if k == late_kind else has

    def comes(k, d, direction):
        has, missing = ((z - d >= 0, missing_up), (z + d < n, missing_down))[direction]
        return has & ~missing if k == late_kind else has

    def rows_of(k, p):
        return sum(pieces[k][:p]), pieces[k][p]

    def load(i):
        k, p = chunks[i]
        start, size = rows_of(k, p)
        return pltpu.make_async_copy(
            w[k].at[pl.ds(start, size)], w_own[k].at[pl.ds(start, size)], load_sem.at[i]
        )

    def side(k):
        return (
            pltpu.make_async_copy(low[k], low_own[k], side_sem.at[0, k]),
            pltpu.make_async_copy(high[k], high_own[k], side_sem.at[1, k]),
        )

    def load_kind(kind):
        for copy in side(kind):
            copy.start()
        for i, (k, p) in enumerate(chunks):
            if k == kind:
                load(i).start()

    barrier = pltpu.get_barrier_semaphore()

    @pl.when(z < middle)
    def _():
        pl.semaphore_signal(barrier, inc=1, device_id={"rows": z + 1}, device_id_type=MESH)

    @pl.when(z > middle)
    def _():
        pl.semaphore_signal(barrier, inc=1, device_id={"rows": z - 1}, device_id_type=MESH)

    @pl.when(top)
    def _():
        for partner in [exchange[0] for exchanges in rounds for exchange in exchanges]:
            pl.semaphore_signal(barrier, inc=1, device_id={"tp": partner}, device_id_type=MESH)

    for kind in order:
        load_kind(kind)

    norm_loads = [
        pltpu.make_async_copy(source, norm_own.at[j], norm_sem.at[j])
        for j, source in enumerate((norm_train, norm_step))
    ]
    for copy in norm_loads:
        copy.start()

    def region(k, p, origin):
        start, size = (0, w[k].shape[0]) if p is None else rows_of(k, p)
        columns = w[k].shape[1]
        if stacked[k]:
            return out[k].at[origin, pl.ds(start, size)]
        if out[k].shape[1] == columns:
            rows = w[k].shape[0]
            return out[k].at[pl.ds(pl.multiple_of(origin * rows + start, 16), size)]
        return out[k].at[pl.ds(start, size), pl.ds(pl.multiple_of(origin * columns, 128), columns)]

    def hop(place, send, recv, direction):
        return pltpu.make_async_remote_copy(
            src_ref=place,
            dst_ref=place,
            send_sem=send,
            recv_sem=recv,
            device_id={"rows": z + 1 - 2 * direction},
            device_id_type=MESH,
        )

    def chunk_hop(i, origin, direction):
        k, p = chunks[i]
        return hop(region(k, p, origin), send_sem.at[direction, i], recv_sem.at[direction, i], direction)

    def whole_hop(k, origin, direction):
        return hop(
            region(k, None, origin),
            pass_send.at[origin, k],
            pass_recv.at[origin, k],
            direction,
        )

    def norm_hop(origin):
        return pltpu.make_async_remote_copy(
            src_ref=norm_all.at[origin, t],
            dst_ref=norm_all.at[origin, t],
            send_sem=norm_send.at[origin],
            recv_sem=norm_recv.at[origin],
            device_id={"rows": z + 1},
            device_id_type=MESH,
        )

    def norm_down():
        return pltpu.make_async_remote_copy(
            src_ref=norm_out,
            dst_ref=norm_out,
            send_sem=down_sem.at[0],
            recv_sem=down_sem.at[1],
            device_id={"rows": z - 1},
            device_id_type=MESH,
        )

    def cross(r, j, coming=False):
        partner, base, theirs, size = rounds[r][j]
        place = norm_all.at[:, pl.ds(theirs if coming else base, size)]
        return pltpu.make_async_remote_copy(
            src_ref=place,
            dst_ref=place,
            send_sem=cross_send.at[r, j],
            recv_sem=cross_recv.at[r, j],
            device_id={"tp": partner},
            device_id_type=MESH,
        )

    def cross_start(r):
        for j in range(len(rounds[r])):
            cross(r, j).start()

    def cross_wait(r):
        for j in range(len(rounds[r])):
            cross(r, j, coming=True).wait_recv()

    def send_greeted(i):
        for direction in range(2):

            @pl.when(sends(chunks[i][0], direction) & greeted[direction])
            def _():
                chunk_hop(i, z, direction).start()

    def send_late():
        for direction in range(2):

            @pl.when(waits[direction])
            def _():
                chunk_hop(0, z + 1 - 2 * direction, 1 - direction).wait_recv()
                if direction == 0:
                    norm_hop(z).start()
                for i, (k, _) in enumerate(chunks):

                    @pl.when(sends(k, direction))
                    def _():
                        chunk_hop(i, z, direction).start()

    def merge(i):
        k, p = chunks[i]
        start, size = rows_of(k, p)
        columns = w[k].shape[1]
        high_block = block_of(size, (160, 128, 64, 32, 16))
        wide_block = block_of(columns, (256, 128))
        wides = columns // wide_block
        place = region(k, p, z)

        def body(b, _):
            if size == high_block:
                r, c = 0, b
            else:
                r, c = b // wides, b % wides
            r = r * high_block
            c = 0 if wides == 1 else pl.multiple_of(c * wide_block, wide_block)
            mine = pl.ds(start + r, high_block)
            wide = pl.ds(c, wide_block)
            result = w_own[k][mine, wide].astype(jnp.float32) + mix_rate * jnp.dot(
                low_rows[k][mine, :], high_own[k][:, wide], preferred_element_type=jnp.float32
            )
            place[pl.ds(r, high_block), wide] = result.astype(jnp.bfloat16)
            return 0

        lax.fori_loop(0, (size // high_block) * wides, body, 0)

    for i, (k, p) in enumerate(chunks):
        if p == 0:
            for copy in side(k):
                copy.wait()
        mine = pl.ds(*rows_of(k, p))
        low_rows[k][mine, :] = low_own[k][:, mine].astype(jnp.float32).T.astype(jnp.bfloat16)
        if i == 1:
            partners = greeted[0].astype(jnp.int32) + greeted[1].astype(jnp.int32)
            partners += top.astype(jnp.int32) * sum(map(len, rounds))

            @pl.when(partners > 0)
            def _():
                pl.semaphore_wait(barrier, partners)

        if i > 0:
            send_greeted(i - 1)
        load(i).wait()
        merge(i)
        if i == min(3, len(chunks) - 2):
            for copy in norm_loads:
                copy.wait()
            norm_all[z, t] = (norm_own[0] + norm_own[1]).astype(jnp.bfloat16).astype(jnp.float32)
        if i == min(4, len(chunks) - 1):

            @pl.when(greeted[0])
            def _():
                norm_hop(z).start()

    send_greeted(len(chunks) - 1)
    send_late()

    def arrival(arrived, onward, d, k, near):
        for direction, origin in ((0, z - d), (1, z + d)):

            @pl.when(comes(k, d, direction))
            def _():
                for j, make in enumerate(arrived):
                    if near and k == order[0] and j == 0:

                        @pl.when(~waits[1 - direction])
                        def _():
                            make(origin, direction).wait_recv()

                    else:
                        make(origin, direction).wait_recv()

                @pl.when(sends(k, direction))
                def _():
                    onward(origin, direction).start()

    def distance(d, _, near=False):
        @pl.when(z - d >= 0)
        def _():
            norm_hop(z - d).wait_recv()

            @pl.when(has_up)
            def _():
                norm_hop(z - d).start()

        for j, k in enumerate(order):

            @pl.when(top & (d == n - 1))
            def _():
                if j == 0:
                    share_norm()
                if j == 1:
                    norm_down().start()

            onward = functools.partial(whole_hop, k)
            arrived = [onward]
            if near:
                arrived = [functools.partial(chunk_hop, i) for i, c in enumerate(chunks) if c[0] == k]
            arrival(arrived, onward, d, k, near)
        return 0

    def share_norm():
        for r in range(len(rounds)):
            cross_start(r)
            cross_wait(r)
        write_norm()

    def write_norm():
        line = jnp.concatenate([norm_all[a, b] for a in range(n) for b in range(tps)], axis=1)
        width = norm_out.shape[1]
        norm_out[...] = jnp.concatenate(
            [line[:, a * width : (a + 1) * width] for a in range(norm_out.shape[0])], axis=0
        ).astype(jnp.bfloat16)

    distance(jnp.int32(1), 0, near=True)
    lax.fori_loop(2, n, distance, 0)

    @pl.when(has_up)
    def _():
        norm_down().wait_recv()

    @pl.when(has_up & has_down)
    def _():
        norm_down().start()

    for direction in range(2):
        for i in range(len(chunks)):

            @pl.when(sends(chunks[i][0], direction))
            def _():
                chunk_hop(i, z, direction).wait_send()

    @pl.when(has_up)
    def _():
        norm_hop(z).wait_send()

    @pl.when(has_down)
    def _():
        norm_down().wait_send()

    def drain(origin, _):
        for direction, passed in ((0, origin < z), (1, origin > z)):
            for k in range(kinds):

                @pl.when(sends(k, direction) & passed)
                def _():
                    whole_hop(k, origin, direction).wait_send()

        @pl.when(has_up & (origin < z))
        def _():
            norm_hop(origin).wait_send()

        return 0

    lax.fori_loop(0, n, drain, 0)

    @pl.when(top)
    def _():
        for r in range(len(rounds)):
            for j in range(len(rounds[r])):
                cross(r, j).wait_send()


def ends(n, units):
    z, late = lax.axis_index("rows"), lax.axis_index("unit") == units - 1
    return late & (z == 0), late & (z == n - 1)


def put(n, units, parts, *refs):
    kinds = len(parts)
    src, dst, sem = refs[:kinds], refs[kinds : 2 * kinds], refs[-1]
    bottom, top = ends(n, units)
    copies, kept = [], []
    for k in range(kinds):
        size = src[k].shape[0] // parts[k]
        for p in range(parts[k]):
            rows = pl.ds(p * size, size)
            copy = pltpu.make_async_copy(src[k].at[rows], dst[k].at[rows], sem.at[len(copies) + len(kept)])
            (kept if k == late_kind else copies).append(copy)
    share = src[late_kind].shape[0] // n

    def own(origin):
        rows = pl.ds(origin * share, share)
        return pltpu.make_async_copy(src[late_kind].at[rows], dst[late_kind].at[rows], sem.at[sum(parts)])

    for copy in copies:
        copy.start()

    @pl.when(~bottom & ~top)
    def _():
        for copy in kept:
            copy.start()
        for copy in kept:
            copy.wait()

    for flag, origin in ((bottom, 0), (top, n - 1)):

        @pl.when(flag)
        def _():
            own(origin).start()
            own(origin).wait()

    for copy in copies:
        copy.wait()


def place(n, units, arrays):
    parts = [2 if x.shape[0] % 128 == 0 else 1 for x in arrays]
    vmem, hbm = pl.BlockSpec(memory_space=pltpu.VMEM), pl.BlockSpec(memory_space=pltpu.HBM)
    return pl.pallas_call(
        functools.partial(put, n, units, parts),
        out_shape=[pltpu.HBM(x.shape, x.dtype) for x in arrays] + [pltpu.VMEM((8, 128), jnp.float32)],
        in_specs=[vmem] * len(arrays),
        out_specs=[hbm] * len(arrays) + [vmem],
        scratch_shapes=[pltpu.SemaphoreType.DMA((sum(parts) + 1,))],
        compiler_params=pltpu.CompilerParams(vmem_limit_bytes=24 * 1024 * 1024),
        name="place",
    )(*arrays)


def last_hop(n, units, have, after, got, send_sem, recv_sem):
    z, late = lax.axis_index("rows"), lax.axis_index("unit") == units - 1
    bottom, top = ends(n, units)
    size = got.shape[0]
    share = have.shape[0] - size

    def hops(direction):
        return [
            pltpu.make_async_remote_copy(
                src_ref=have.at[pl.ds(share * (direction + j), share)],
                dst_ref=got.at[pl.ds(share * j, share)],
                send_sem=send_sem.at[direction, j],
                recv_sem=recv_sem.at[direction, j],
                device_id={"rows": z + 1 - 2 * direction},
                device_id_type=MESH,
            )
            for j in range(n - 1)
        ]

    barrier = pltpu.get_barrier_semaphore()
    above, below = late & (z == n - 2), late & (z == 1)

    @pl.when(bottom)
    def _():
        pl.semaphore_signal(barrier, inc=1, device_id={"rows": z + 1}, device_id_type=MESH)

    @pl.when(top)
    def _():
        pl.semaphore_signal(barrier, inc=1, device_id={"rows": z - 1}, device_id_type=MESH)

    @pl.when(above | below)
    def _():
        pl.semaphore_wait(barrier, above.astype(jnp.int32) + below.astype(jnp.int32))

    for direction, flag in ((0, above), (1, below)):

        @pl.when(flag)
        def _():
            for hop in hops(direction):
                hop.start()

    for direction, flag in ((0, top), (1, bottom)):

        @pl.when(flag)
        def _():
            for hop in hops(direction):
                hop.wait_recv()

    for direction, flag in ((0, above), (1, below)):

        @pl.when(flag)
        def _():
            for hop in hops(direction):
                hop.wait_send()


def finish(n, units, have, after):
    share = have.shape[0] // n
    vmem, dma = pl.BlockSpec(memory_space=pltpu.VMEM), pltpu.SemaphoreType.DMA
    return pl.pallas_call(
        functools.partial(last_hop, n, units),
        out_shape=pltpu.VMEM((have.shape[0] - share, have.shape[1]), have.dtype),
        in_specs=[vmem, vmem],
        out_specs=vmem,
        scratch_shapes=[dma((2, n - 1)), dma((2, n - 1))],
        compiler_params=pltpu.CompilerParams(
            collective_id=1, has_side_effects=True, vmem_limit_bytes=4 * 1024 * 1024
        ),
        name="last_hop",
    )(have, after)


def add_rows(n, units, got, old, out, sem):
    size = got.shape[0]
    share = out.shape[0] - size
    for flag, start in zip(ends(n, units), (share, 0)):

        @pl.when(flag)
        def _():
            copies = [
                pltpu.make_async_copy(
                    got.at[pl.ds(j * share, share)], out.at[pl.ds(start + j * share, share)], sem.at[j]
                )
                for j in range(n - 1)
            ]
            for copy in copies:
                copy.start()
            for copy in copies:
                copy.wait()


def complete(n, units, got, old):
    vmem, hbm = pl.BlockSpec(memory_space=pltpu.VMEM), pl.BlockSpec(memory_space=pltpu.HBM)
    return pl.pallas_call(
        functools.partial(add_rows, n, units),
        out_shape=pltpu.HBM(old.shape, old.dtype),
        in_specs=[vmem, hbm],
        out_specs=hbm,
        scratch_shapes=[pltpu.SemaphoreType.DMA((n - 1,))],
        input_output_aliases={1: 0},
        compiler_params=pltpu.CompilerParams(vmem_limit_bytes=4 * 1024 * 1024),
        name="complete",
    )(got, old)


def shards(n, tps, units, *args):
    w, low, high = args[0:12:3], [x.T for x in args[1:12:3]], args[2:12:3]
    norm_train, norm_step = args[12].reshape(1, -1), args[13].reshape(1, -1)
    kinds = len(w)
    by_column = [False] * (kinds - 1) + [True]
    stacked = [by_column[k] and w[k].shape[1] % 128 != 0 for k in range(kinds)]
    firsts = {order[0]: (128, 128), order[1]: ()}
    pieces = [pieces_of(w[k].shape[0], firsts.get(k, ())) for k in range(kinds)]
    count = sum(map(len, pieces))
    rounds = rounds_of(tps, 0)
    crossings = (len(rounds), max(map(len, rounds), default=0))
    shapes = []
    for k in range(kinds):
        rows, columns = w[k].shape
        if stacked[k]:
            shapes.append((n, rows, columns))
        elif by_column[k]:
            shapes.append((rows, n * columns))
        else:
            shapes.append((n * rows, columns))
    share = norm_train.shape[1]
    total = n * tps * share
    width = 128 if total % 128 == 0 else total
    vmem, hbm = pl.BlockSpec(memory_space=pltpu.VMEM), pl.BlockSpec(memory_space=pltpu.HBM)
    dma = pltpu.SemaphoreType.DMA
    operands = (*w, *low, *high, norm_train, norm_step)
    results = pl.pallas_call(
        functools.partial(kernel, n, tps, units, stacked, pieces),
        out_shape=[pltpu.VMEM(s, jnp.bfloat16) for s in shapes]
        + [pltpu.VMEM((total // width, width), jnp.bfloat16)],
        in_specs=[hbm] * (3 * kinds + 2),
        out_specs=[vmem] * (kinds + 1),
        scratch_shapes=[pltpu.VMEM(x.shape, x.dtype) for x in (*w, *low, *high)]
        + [pltpu.VMEM(x.shape[::-1], x.dtype) for x in low]
        + [
            pltpu.VMEM((2, 1, share), jnp.float32),
            pltpu.VMEM((n, tps, 1, share), jnp.float32),
            dma((2,)),
            dma((count,)),
            dma((2, kinds)),
            dma((2, count)),
            dma((2, count)),
            dma((n, kinds)),
            dma((n, kinds)),
            dma((n,)),
            dma((n,)),
            dma((2,)),
            dma(crossings),
            dma(crossings),
        ],
        compiler_params=pltpu.CompilerParams(
            collective_id=0, has_side_effects=True, vmem_limit_bytes=24 * 1024 * 1024
        ),
        name="merge_and_gather",
    )(*[pltpu.with_memory_space_constraint(x, pltpu.HBM) for x in operands])
    have = results[late_kind]
    *results, after = place(n, units, results)
    if n > 1:
        results[late_kind] = complete(n, units, finish(n, units, have, after), results[late_kind])
    finals = []
    for k in range(kinds):
        full = results[k]
        if stacked[k]:
            full = full.transpose(1, 0, 2).reshape(full.shape[1], -1)
        finals.append(full)
    return (*finals, results[kinds].reshape(-1))


def solution(mesh):
    return jax.shard_map(
        functools.partial(shards, mesh.shape["rows"], mesh.shape["tp"], mesh.shape["unit"]),
        mesh=mesh,
        in_specs=(
            P(("unit", "rows"), "tp"),
            P(("unit", "rows"), None),
            P("unit", "tp"),
            P(("unit", "rows"), "tp"),
            P(("unit", "rows"), None),
            P("unit", "tp"),
            P(("unit", "rows"), "tp"),
            P(("unit", "rows"), None),
            P("unit", "tp"),
            P(("unit", "tp"), "rows"),
            P(("unit", "tp"), None),
            P("unit", "rows"),
            P(("unit", "rows", "tp")),
            P(("unit", "rows", "tp")),
        ),
        out_specs=(
            P("unit", "tp"),
            P("unit", "tp"),
            P("unit", "tp"),
            P(("unit", "tp"), None),
            P("unit"),
        ),
        check_vma=False,
    )
```
